256 devices in a mesh: dp: 2 (over core), section: 8 (over z), mp: 16 (over y, x).
Axes of the slice: x: 4, y: 4, z: 8, core: 2. Of those that a mesh axis runs over, the one named last changes fastest.
Arguments:
- inputs: bfloat16 [192, 512], P(('dp', 'mp')), may hold values from -6 to 6
- tangents: bfloat16 [192, 32, 512], P(('dp', 'mp')), may hold values from -6 to 6
- targets: bfloat16 [192, 1024], P(('dp', 'mp')), may hold values from -24 to 24
- target_jac: bfloat16 [192, 32, 1024], P(('dp', 'mp')), may hold values from -24 to 24
- rank_mask: int32 [192, 32], P(('dp', 'mp')), may hold values from 0 to 1, as said below
- batch_order: int32 [32, 6], P(('dp', 'mp')), may hold values from 0 to 5, each once within a row
- encoder: bfloat16 [512, 2048], replicated, may hold values from -0.25 to 0.25
- layers: bfloat16 [8, 2048, 2048], P('section', 'mp'), may hold values from -0.125 to 0.125
- head_weight: bfloat16 [2048, 1024], replicated, may hold values from -0.125 to 0.125
Outputs:
- grad_layers: float32 [8, 2048, 2048], P('section', ('dp', 'mp'))
- grad_head: float32 [2048, 1024], P(('dp', 'mp'), 'section')
- loss_value: float32 [], replicated
The draws below stay inside these ranges and needn't reach their ends.
Inputs may be any that keep to these rules, and one draw needn't show every extreme that they name: `rank_mask`: each sample's ones are its first 1 to 32 directions. `batch_order`: each row is an ordering of 0 .. 5.
All inputs are finite; a program needn't handle non-finite values.
Results may differ from the reference program's by a relative error of at most 0.035.
Values may be sent and summed in bfloat16 or wider, within the bound.
A program may use at most 128 MiB of HBM per device.

```python
import jax
import jax.numpy as jnp
from jax import lax

D = 2048
DIN = 512
DOUT = 1024
RANK = 32
MB = 6
S_DEV = 1
SAMP_DEV = 6
GROUP_ROWS = 32
SAMPLES = 192
LAYERS = 8
N_DP = 2
N_MP = 16


def draw_rank_mask(key, part):
    jitter_key = jax.random.fold_in(key, 12)
    device_rows = jnp.arange(GROUP_ROWS, dtype=jnp.int32)[:, None]
    model_index = device_rows % N_MP
    base_rank = 1 + (RANK - 1) * model_index // max(N_MP - 1, 1)
    jitter = jax.random.randint(jitter_key, (GROUP_ROWS, SAMP_DEV), -1, 2)
    active = jnp.clip(base_rank + jitter, 1, RANK)
    last_row = jnp.arange(SAMP_DEV, dtype=jnp.int32)[None, :] == 0
    active = jnp.where((model_index == N_MP - 1) & last_row, RANK, active).reshape(SAMPLES, 1)
    return (jnp.arange(RANK, dtype=jnp.int32)[None, :] < active).astype(jnp.int32)


def row_scales(key):
    scale_key = jax.random.fold_in(key, 21)
    device_rows = jnp.arange(GROUP_ROWS, dtype=jnp.float32) / max(GROUP_ROWS - 1, 1)
    wobble = jax.random.uniform(scale_key, (GROUP_ROWS,), jnp.float32, -0.1, 0.1)
    low_end = jnp.log(0.3)
    high_end = jnp.log(3.9)
    return jnp.exp(low_end + (high_end - low_end) * device_rows + wobble)


def draw_targets(key, part):
    value_key = jax.random.fold_in(key, 22)
    scales = row_scales(key)[:, None, None]
    values = jnp.clip(jax.random.normal(value_key, (GROUP_ROWS, SAMP_DEV, DOUT), jnp.float32), -6.0, 6.0)
    return jnp.clip(scales * values, -24.0, 24.0).reshape(SAMPLES, DOUT).astype(jnp.bfloat16)


def draw_target_jac(key, part):
    value_key = jax.random.fold_in(key, 23)
    scales = row_scales(key)[:, None, None, None]
    shape = (GROUP_ROWS, SAMP_DEV, RANK, DOUT)
    values = jnp.clip(jax.random.normal(value_key, shape, jnp.float32), -6.0, 6.0)
    return jnp.clip(scales * values, -24.0, 24.0).reshape(SAMPLES, RANK, DOUT).astype(jnp.bfloat16)


def steps_of(own_key, extent, cuts, least, top_value):
    level, own = 1.0, jax.random.fold_in(own_key, 6)
    for axis_at, blocks in cuts:
        draws = jnp.exp(jax.random.uniform(jax.random.fold_in(own, axis_at), (blocks,), jnp.float32, least / len(cuts), top_value / len(cuts)))
        level = level * jnp.repeat(draws, extent[axis_at] // blocks).reshape([-1 if axis == axis_at else 1 for axis in range(len(extent))])
    return level


def normal_values(rng, shape, spread, limit, pieces=(), held_as=jnp.bfloat16):
    result = jax.random.normal(rng, shape, jnp.float32) * spread
    if len(pieces) > 0:
        result = steps_of(rng, shape, pieces, -0.22, 0.18) * result
    return jnp.clip(result, min=-limit, max=limit).astype(held_as)


def setup_inputs(seed: int = 0) -> dict:
    streams_of = jax.random.split(jax.random.key(seed), 10)
    return {
        "inputs": normal_values(streams_of[0], (SAMPLES, DIN), 1.0, 6.0, ((0, 32),)),
        "tangents": normal_values(streams_of[1], (SAMPLES, RANK, DIN), 1.0, 6.0, ((0, 32),)),
        "targets": draw_targets(jax.random.fold_in(streams_of[9], 71), 0),
        "target_jac": draw_target_jac(jax.random.fold_in(streams_of[9], 71), 0),
        "rank_mask": draw_rank_mask(jax.random.fold_in(streams_of[9], 71), 0),
        "batch_order": jax.vmap(lambda own: jax.random.permutation(own, SAMP_DEV))(jax.random.split(streams_of[5], GROUP_ROWS)).reshape((GROUP_ROWS, SAMP_DEV)).astype(jnp.int32),
        "encoder": normal_values(streams_of[6], (DIN, D), DIN ** -0.5, 0.25),
        "layers": normal_values(streams_of[7], (LAYERS, D, D), D ** -0.5, 0.125, ((0, 8), (1, 16))),
        "head_weight": normal_values(streams_of[8], (D, DOUT), D ** -0.5, 0.125),
    }


def forward_layer(row_block, weight):
    model_width = weight.shape[1]
    pre_act = jnp.dot(row_block.reshape(-1, model_width), weight, preferred_element_type=jnp.float32).reshape(row_block.shape)
    tanh_p = jnp.tanh(pre_act[:, 0])
    slope_vals = 1.0 - tanh_p * tanh_p
    primal = row_block[:, 0].astype(jnp.float32) + tanh_p
    tangent = row_block[:, 1:].astype(jnp.float32) + slope_vals[:, None, :] * pre_act[:, 1:]
    return jnp.concatenate([primal[:, None], tangent], axis=1).astype(jnp.bfloat16), pre_act


def backward_layer(row_block, pre_act, grad_rows, weight):
    model_width = weight.shape[1]
    upstream = grad_rows.astype(jnp.float32)
    tanh_p = jnp.tanh(pre_act[:, 0])
    slope_vals = 1.0 - tanh_p * tanh_p
    tangent_part = upstream[:, 1:] * slope_vals[:, None, :]
    slope_grad = jnp.sum(upstream[:, 1:] * pre_act[:, 1:], axis=1)
    primal_part = upstream[:, 0] * slope_vals - 2.0 * slope_grad * tanh_p * slope_vals
    grad_mix = jnp.concatenate([primal_part[:, None], tangent_part], axis=1).astype(jnp.bfloat16)
    back_rows = jnp.dot(grad_mix.reshape(-1, model_width), weight.T, preferred_element_type=jnp.float32).reshape(upstream.shape)
    return grad_mix, (upstream + back_rows).astype(jnp.bfloat16)


def block_sum(left, right):
    blocks = (left.reshape(N_DP * N_MP, -1, left.shape[-1]), right.reshape(N_DP * N_MP, -1, right.shape[-1]))

    def add_block(running, block_pair):
        partial_value = jnp.dot(block_pair[0].T, block_pair[1], preferred_element_type=jnp.float32)
        rounded = lax.optimization_barrier(partial_value.astype(jnp.bfloat16))
        return running + rounded.astype(jnp.float32), None

    running, _ = lax.scan(add_block, jnp.zeros((left.shape[-1], right.shape[-1]), jnp.float32), blocks)
    return running


def reference(inputs, tangents, targets, target_jac, rank_mask, batch_order, encoder, layers, head_weight):
    row_depth = RANK + 1
    rows_in = jnp.concatenate([inputs[:, None, :], tangents], axis=1)
    hidden = jnp.dot(rows_in.reshape(-1, DIN), encoder, preferred_element_type=jnp.float32).reshape(SAMPLES, row_depth, D).astype(jnp.bfloat16)
    saved_in = []
    saved_pre = []
    for layer_idx in range(LAYERS):
        saved_in.append(hidden)
        hidden, pre_act = forward_layer(hidden, layers[layer_idx])
        saved_pre.append(pre_act)
    outputs = jnp.dot(hidden.reshape(-1, D), head_weight, preferred_element_type=jnp.float32).reshape(SAMPLES, row_depth, DOUT)
    row_weight = jnp.concatenate([jnp.ones((SAMPLES, 1), jnp.float32), rank_mask.astype(jnp.float32)], axis=1)
    wanted = jnp.concatenate([targets[:, None, :], target_jac], axis=1).astype(jnp.float32)
    mismatch = outputs - wanted
    misfit = jnp.sum(row_weight[:, :, None] * mismatch * mismatch, axis=(1, 2))
    sample_index = (jnp.arange(GROUP_ROWS, dtype=jnp.int32)[:, None] * SAMP_DEV + batch_order).reshape(-1)
    batch_id = ((jnp.arange(GROUP_ROWS, dtype=jnp.int32)[:, None] // N_MP) * MB + (jnp.arange(SAMP_DEV, dtype=jnp.int32) // S_DEV)[None, :]).reshape(-1)
    micro_of = jnp.zeros((SAMPLES,), jnp.int32).at[sample_index].set(batch_id.astype(jnp.int32))
    totals = jax.ops.segment_sum(jnp.sum(row_weight, axis=1), micro_of, num_segments=N_DP * MB)
    divisor = totals[micro_of]
    loss_value = jnp.sum(misfit / divisor) / (N_DP * MB * DOUT)
    cot_out = (2.0 * row_weight[:, :, None] * mismatch / divisor[:, None, None]).astype(jnp.bfloat16)
    grad_head = block_sum(hidden, cot_out)
    grad_rows = jnp.dot(cot_out.reshape(-1, DOUT), head_weight.T, preferred_element_type=jnp.float32).reshape(SAMPLES, row_depth, D).astype(jnp.bfloat16)
    layer_grads = [None] * LAYERS
    for layer_idx in reversed(range(LAYERS)):
        grad_mix, grad_rows = backward_layer(saved_in[layer_idx], saved_pre[layer_idx], grad_rows, layers[layer_idx])
        layer_grads[layer_idx] = block_sum(saved_in[layer_idx], grad_mix)
    return jnp.stack(layer_grads), grad_head, loss_value
```

```python
import functools

import jax
import jax.numpy as jnp
from jax import lax
from jax.experimental import pallas as pl
from jax.experimental.pallas import tpu as pltpu
from jax.sharding import PartitionSpec as P

MB = 6
ROWS = 48
MESH = pl.DeviceIdType.MESH


def first_row(row, height):
    rows = lax.broadcasted_iota(jnp.int32, (height, row.shape[1]), 0)
    return jnp.where(rows == 0, jnp.broadcast_to(row, (height, row.shape[1])), 0.0)


def relay_kernel(
    sections, pieces,
    h0, h0p, w, head, head_t, want, coef,
    o_in, o_mix, o_out, o_cot, o_loss,
    xin, pin, pout, pre, thb, cin, cpin, cout, cpout,
    fsend, frecv, bsend, brecv,
):
    n_mb, rows, width = xin.shape
    rank = cin.shape[1]
    out_width = head.shape[1]
    tile = width // pieces
    s = lax.axis_index("section")
    nxt = lax.rem(s + 1, sections)
    prv = lax.rem(s + sections - 1, sections)
    first = s == 0
    last = s == sections - 1

    barrier = pltpu.get_barrier_semaphore()
    for other in (nxt, prv):
        pl.semaphore_signal(barrier, inc=1, device_id={"section": other}, device_id_type=MESH)
    pl.semaphore_wait(barrier, 2)

    def fcopy(m, j):
        cols = pl.ds(j * tile, tile)
        return pltpu.make_async_remote_copy(
            src_ref=o_out.at[m, pl.ds(0, rank), cols],
            dst_ref=xin.at[m, pl.ds(0, rank), cols],
            send_sem=fsend.at[m, j], recv_sem=frecv.at[m, j],
            device_id={"section": nxt}, device_id_type=MESH,
        )

    def fpcopy(m):
        return pltpu.make_async_remote_copy(
            src_ref=pout.at[m], dst_ref=pin.at[m],
            send_sem=fsend.at[m, pieces], recv_sem=frecv.at[m, pieces],
            device_id={"section": nxt}, device_id_type=MESH,
        )

    def bcopy(m, j):
        cols = pl.ds(j * tile, tile)
        return pltpu.make_async_remote_copy(
            src_ref=cout.at[m, :, cols], dst_ref=cin.at[m, :, cols],
            send_sem=bsend.at[m, j], recv_sem=brecv.at[m, j],
            device_id={"section": prv}, device_id_type=MESH,
        )

    def bpcopy(m):
        return pltpu.make_async_remote_copy(
            src_ref=cpout.at[m], dst_ref=cpin.at[m],
            send_sem=bsend.at[m, pieces], recv_sem=brecv.at[m, pieces],
            device_id={"section": prv}, device_id_type=MESH,
        )

    @pl.when(first)
    def _():
        xin[...] = h0[...]
        pin[...] = h0p[...]

    def forward(m, _):
        @pl.when(jnp.logical_not(first))
        def _():
            for j in range(pieces):
                fcopy(m, j).wait_recv()
            fpcopy(m).wait_recv()
            xin[m, pl.ds(rank, rows - rank), :] = first_row(pin[m], rows - rank).astype(jnp.bfloat16)

        for j in range(pieces):
            cols = pl.ds(j * tile, tile)
            acc = jnp.dot(xin[m], w[:, cols], preferred_element_type=jnp.float32)
            th = jnp.tanh(acc[rank : rank + 1, :])
            slope = 1.0 - th * th
            tangent = acc[:rank, :]
            pre[m, :, cols] = tangent
            thb[m, :, cols] = th
            moved = xin[m, pl.ds(0, rank), cols].astype(jnp.float32) + slope * tangent
            o_out[m, pl.ds(0, rank), cols] = moved.astype(jnp.bfloat16)
            primal = (pin[m, :, cols] + th).astype(jnp.bfloat16).astype(jnp.float32)
            pout[m, :, cols] = primal
            o_out[m, pl.ds(rank, rows - rank), cols] = first_row(primal, rows - rank).astype(jnp.bfloat16)

            @pl.when(jnp.logical_not(last))
            def _():
                fcopy(m, j).start()

        @pl.when(jnp.logical_not(last))
        def _():
            fpcopy(m).start()

        return 0

    lax.fori_loop(0, n_mb, forward, 0)

    @pl.when(jnp.logical_not(last))
    def _():
        o_cot[...] = jnp.zeros_like(o_cot)
        o_loss[...] = jnp.zeros_like(o_loss)

    @pl.when(last)
    def _():
        step = 256 if out_width % 256 == 0 else out_width
        total = jnp.zeros((1, 1), jnp.float32)
        scale = coef[...]
        for n in range(out_width // step):
            cols = pl.ds(n * step, step)
            outputs = jnp.dot(
                o_out[...].reshape(n_mb * rows, width), head[:, cols],
                preferred_element_type=jnp.float32,
            )
            mismatch = outputs - want[:, cols].astype(jnp.float32)
            weighted = scale * mismatch
            total = total + jnp.sum(
                jnp.sum(weighted * mismatch, axis=0, keepdims=True), axis=1, keepdims=True
            )
            o_cot[:, cols] = (2.0 * weighted).astype(jnp.bfloat16)
        o_loss[...] = jnp.broadcast_to(total, o_loss.shape)
        for n in range(width // step):
            cols = pl.ds(n * step, step)
            grads = jnp.dot(o_cot[...], head_t[:, cols], preferred_element_type=jnp.float32)
            grads = grads.astype(jnp.bfloat16)
            for m in range(n_mb):
                cin[m, :, cols] = grads[m * rows : m * rows + rank, :]
                cpin[m, :, cols] = grads[m * rows + rank : m * rows + rows, :].astype(jnp.float32)[0:1]

    def backward(m, _):
        @pl.when(jnp.logical_not(last))
        def _():
            for j in range(pieces):
                bcopy(m, j).wait_recv()
            bpcopy(m).wait_recv()

        for j in range(pieces):
            cols = pl.ds(j * tile, tile)
            upstream = cin[m, :, cols].astype(jnp.float32)
            th = thb[m, :, cols]
            slope = 1.0 - th * th
            o_mix[m, pl.ds(0, rank), cols] = (upstream * slope).astype(jnp.bfloat16)
            total = jnp.sum(upstream * pre[m, :, cols], axis=0, keepdims=True)
            primal = cpin[m, :, cols] * slope - 2.0 * total * th * slope
            o_mix[m, pl.ds(rank, rows - rank), cols] = first_row(primal, rows - rank).astype(jnp.bfloat16)

        @pl.when(jnp.logical_not(first))
        def _():
            for j in range(pieces):
                cols = pl.ds(j * tile, tile)
                back = lax.dot_general(
                    o_mix[m], w[cols, :], (((1,), (1,)), ((), ())),
                    preferred_element_type=jnp.float32,
                )
                cout[m, :, cols] = (cin[m, :, cols].astype(jnp.float32) + back[:rank]).astype(jnp.bfloat16)
                cpout[m, :, cols] = (
                    (cpin[m, :, cols] + back[rank : rank + 1]).astype(jnp.bfloat16).astype(jnp.float32)
                )
                bcopy(m, j).start()
            bpcopy(m).start()

        return 0

    lax.fori_loop(0, n_mb, backward, 0)
    o_in[...] = xin[...]

    def drain(m, _):
        @pl.when(jnp.logical_not(last))
        def _():
            for j in range(pieces):
                fcopy(m, j).wait_send()
            fpcopy(m).wait_send()

        @pl.when(jnp.logical_not(first))
        def _():
            for j in range(pieces):
                bcopy(m, j).wait_send()
            bpcopy(m).wait_send()

        return 0

    lax.fori_loop(0, n_mb, drain, 0)


def relay(sections, h0, h0p, w, head, head_t, want, coef):
    n_mb, rows, width = h0.shape
    rank = 32
    out_width = head.shape[1]
    pieces = 4
    bf16, f32 = jnp.bfloat16, jnp.float32
    vmem = pl.BlockSpec(memory_space=pltpu.VMEM)
    return pl.pallas_call(
        functools.partial(relay_kernel, sections, pieces),
        out_shape=(
            jax.ShapeDtypeStruct((n_mb, rows, width), bf16),
            jax.ShapeDtypeStruct((n_mb, rows, width), bf16),
            jax.ShapeDtypeStruct((n_mb, rows, width), bf16),
            jax.ShapeDtypeStruct((n_mb * rows, out_width), bf16),
            jax.ShapeDtypeStruct((8, 128), f32),
        ),
        in_specs=[vmem] * 7,
        out_specs=(vmem,) * 5,
        scratch_shapes=[
            pltpu.VMEM((n_mb, rows, width), bf16),
            pltpu.VMEM((n_mb, 1, width), f32),
            pltpu.VMEM((n_mb, 1, width), f32),
            pltpu.VMEM((n_mb, rank, width), f32),
            pltpu.VMEM((n_mb, 1, width), f32),
            pltpu.VMEM((n_mb, rank, width), bf16),
            pltpu.VMEM((n_mb, 1, width), f32),
            pltpu.VMEM((n_mb, rank, width), bf16),
            pltpu.VMEM((n_mb, 1, width), f32),
            pltpu.SemaphoreType.DMA((n_mb, pieces + 1)),
            pltpu.SemaphoreType.DMA((n_mb, pieces + 1)),
            pltpu.SemaphoreType.DMA((n_mb, pieces + 1)),
            pltpu.SemaphoreType.DMA((n_mb, pieces + 1)),
        ],
        compiler_params=pltpu.CompilerParams(
            collective_id=0, has_side_effects=True, vmem_limit_bytes=60 * 1024 * 1024
        ),
        name="relay",
    )(h0, h0p, w, head, head_t, want, coef)


def sample_rows(primal, tangents):
    count, rank, width = tangents.shape
    zeros = jnp.zeros((count, ROWS - rank - 1, width), tangents.dtype)
    return jnp.concatenate([tangents, primal[:, None], zeros], axis=1)


def local(
    inputs, tangents, targets, target_jac, rank_mask, batch_order, encoder, layers, head_weight
):
    samples, rank, in_width = tangents.shape
    width = layers.shape[2]
    out_width = head_weight.shape[1]
    sections = lax.axis_size("section")
    f32 = jnp.float32
    weight = lax.all_gather(layers[0], "mp", axis=0, tiled=True)

    mask = rank_mask.astype(f32)
    totals = 1.0 + jnp.sum(mask, axis=1)
    here = (batch_order[0][:, None] == jnp.arange(samples)[None, :]).astype(f32)
    counts = lax.psum(jnp.sum(here * totals[None, :], axis=1), "mp")
    count_of = jnp.sum(here * counts[:, None], axis=0)
    row_weight = jnp.concatenate(
        [mask, jnp.ones((samples, 1), f32), jnp.zeros((samples, ROWS - rank - 1), f32)], axis=1
    )
    coef = (row_weight / count_of[:, None]).reshape(samples * ROWS, 1)

    rows_in = sample_rows(inputs, tangents).reshape(samples * ROWS, in_width)
    lifted = jnp.dot(rows_in, encoder, preferred_element_type=f32).astype(jnp.bfloat16)
    h0 = lifted.reshape(samples, ROWS, width)
    h0p = h0[:, rank : rank + 1].astype(f32)
    want = sample_rows(targets, target_jac).reshape(samples * ROWS, out_width)

    x_in, mix, x_out, cot, loss = relay(
        sections, h0, h0p, weight, head_weight, head_weight.T, want, coef
    )
    flat = lambda a: a.reshape(samples * ROWS, -1)
    grad_layer = jnp.dot(flat(x_in).T, flat(mix), preferred_element_type=f32)
    grad_head = jnp.dot(flat(x_out).T, cot, preferred_element_type=f32)
    both = jnp.concatenate([grad_layer.astype(jnp.bfloat16), grad_head.astype(jnp.bfloat16)], axis=1)
    summed = lax.psum_scatter(both, ("dp", "mp"), scatter_dimension=0, tiled=True)
    grad_layers = summed[:, :width].astype(f32)[None]
    parts = jnp.moveaxis(summed[:, width:].reshape(summed.shape[0], sections, -1), 1, 0)
    arrived = lax.all_to_all(parts, "section", split_axis=0, concat_axis=0, tiled=True)
    grad_head_out = arrived[sections - 1].astype(f32)
    loss_sum = lax.psum(loss[0, 0], ("dp", "section", "mp"))
    loss_value = loss_sum / (lax.axis_size("dp") * MB * out_width)
    return grad_layers, grad_head_out, loss_value


def solution(mesh):
    in_specs = (
        P(("dp", "mp"), None),
        P(("dp", "mp"), None, None),
        P(("dp", "mp"), None),
        P(("dp", "mp"), None, None),
        P(("dp", "mp"), None),
        P(("dp", "mp"), None),
        P(),
        P("section", "mp", None),
        P(),
    )
    out_specs = (P("section", ("dp", "mp"), None), P(("dp", "mp"), "section"), P())
    return jax.shard_map(local, mesh=mesh, in_specs=in_specs, out_specs=out_specs, check_vma=False)
```

```python
import functools

import jax
import jax.numpy as jnp
from jax import lax
from jax.experimental import pallas as pl
from jax.experimental.pallas import tpu as pltpu
from jax.sharding import PartitionSpec as P

SIDE = 4
ROWS = 48
PIECES = 4
MESH = pl.DeviceIdType.MESH
BF16, F32 = jnp.bfloat16, jnp.float32


def first_row(row, height):
    rows = lax.broadcasted_iota(jnp.int32, (height, row.shape[1]), 0)
    return jnp.where(rows == 0, jnp.broadcast_to(row, (height, row.shape[1])), 0.0)


def stacked_rows(get_row, count, height, width):
    rows = lax.broadcasted_iota(jnp.int32, (height, width), 0)
    block = jnp.zeros((height, width), F32)
    for m in range(count):
        block = jnp.where(rows == m, jnp.broadcast_to(get_row(m), (height, width)), block)
    return block


class Place:
    def __init__(self, sections):
        self.sections = sections
        self.core = lax.axis_index("dp")
        self.s = lax.axis_index("section")
        self.mp = lax.axis_index("mp")
        self.y = self.mp // SIDE
        self.x = lax.rem(self.mp, SIDE)
        self.first = self.s == 0
        self.last = self.s == sections - 1
        self.nxt = lax.rem(self.s + 1, sections)
        self.prv = lax.rem(self.s + sections - 1, sections)

    def along(self, coordinate, steps):
        return lax.rem(coordinate + steps + SIDE, SIDE)

    def chip(self, axis, steps):
        if axis == 0:
            return self.y * SIDE + self.along(self.x, steps)
        return self.along(self.y, steps) * SIDE + self.x


def remote(src, dst, send, recv, device_id):
    return pltpu.make_async_remote_copy(
        src_ref=src, dst_ref=dst, send_sem=send, recv_sem=recv,
        device_id=device_id, device_id_type=MESH,
    )


def enter(place):
    barrier = pltpu.get_barrier_semaphore()
    plane = 2 * SIDE * SIDE
    me = place.core * (SIDE * SIDE) + place.mp

    def tell_plane(step, _):
        other = lax.rem(me + step, plane)
        pl.semaphore_signal(
            barrier, inc=1,
            device_id={"dp": other // (SIDE * SIDE), "mp": lax.rem(other, SIDE * SIDE)},
            device_id_type=MESH,
        )
        return 0

    def tell_column(step, _):
        other = lax.rem(place.s + step, place.sections)
        pl.semaphore_signal(barrier, inc=1, device_id={"section": other}, device_id_type=MESH)
        return 0

    lax.fori_loop(1, plane, tell_plane, 0)
    lax.fori_loop(1, place.sections, tell_column, 0)
    pl.semaphore_wait(barrier, plane - 1 + place.sections - 1)


class Gather:
    def __init__(self, place, shard, w, sems):
        self.p, self.shard, self.w = place, shard, w
        self.send1, self.recv1, self.send2, self.recv2 = sems[:4]
        self.dsend1, self.drecv1, self.dsend2, self.drecv2 = sems[4:]
        self.depth = shard.shape[0]
        self.piece = self.depth // 4

    def rows(self, q, core, step1, step2, half):
        p = self.p
        dx, dy = (step1, step2) if q == 0 else (step2, step1)
        chip = p.along(p.y, dy) * SIDE + p.along(p.x, dx)
        start = chip * self.depth + core * (2 * self.piece) + q * self.piece
        length = self.piece
        if half is not None:
            length = self.piece // 2
            start = start + half * length
        return pl.ds(pl.multiple_of(start, length), length)

    def copy(self, q, phase, o, e):
        p = self.p
        axis = q if phase == 1 else 1 - q
        to = 1 if e in (0, 2) else -1
        back = {0: 0, 1: 0, 2: -1, 3: 1}[e]
        half = {0: None, 1: None, 2: 0, 3: 1}[e]
        step1, step2 = (back, 0) if phase == 1 else (o, back)
        dst = self.w.at[self.rows(q, p.core, step1, step2, half)]
        src = dst
        if step1 == 0 and step2 == 0:
            src = self.shard.at[pl.ds(pl.multiple_of(p.core * (2 * self.piece) + q * self.piece, self.piece), self.piece)]
        send, recv = self.sems(phase, q, o, e, self.send1, self.recv1, self.send2, self.recv2)
        return remote(src, dst, send, recv, {"mp": p.chip(axis, to)})

    def sems(self, phase, q, o, e, send1, recv1, send2, recv2):
        if phase == 1:
            return send1.at[q, e], recv1.at[q, e]
        return send2.at[q, o % SIDE, e], recv2.at[q, o % SIDE, e]

    def arrived(self, q, phase, o, e):
        p = self.p
        away = {0: -1, 1: 1, 2: -2, 3: 2}[e]
        half = {0: None, 1: None, 2: 0, 3: 1}[e]
        step1, step2 = (away, 0) if phase == 1 else (o, away)
        return self.p, q, step1, step2, half

    def wait(self, q, phase, o, e):
        p, q, step1, step2, half = self.arrived(q, phase, o, e)
        dst = self.w.at[self.rows(q, p.core, step1, step2, half)]
        send, recv = self.sems(phase, q, o, e, self.send1, self.recv1, self.send2, self.recv2)
        remote(dst, dst, send, recv, {"mp": p.chip(0, 1)}).wait_recv()
        self.across(q, phase, o, e, p.core).start()

    def across(self, q, phase, o, e, core):
        p, q, step1, step2, half = self.arrived(q, phase, o, e)
        ref = self.w.at[self.rows(q, core, step1, step2, half)]
        send, recv = self.sems(phase, q, o, e, self.dsend1, self.drecv1, self.dsend2, self.drecv2)
        return remote(ref, ref, send, recv, {"dp": 1 - p.core})

    def begin(self):
        for q in (0, 1):
            self.copy(q, 1, 0, 0).start()
            self.copy(q, 1, 0, 1).start()
        for q in (0, 1):
            self.copy(q, 2, 0, 0).start()
            self.copy(q, 2, 0, 1).start()
        p = self.p
        self.w[pl.ds(pl.multiple_of(p.mp * self.depth, self.depth), self.depth), :] = self.shard[...]

    def run(self):
        for q in (0, 1):
            self.wait(q, 1, 0, 0)
            self.copy(q, 1, 0, 2).start()
            self.wait(q, 1, 0, 1)
            self.copy(q, 1, 0, 3).start()
        for q in (0, 1):
            for o in (-1, 1):
                self.copy(q, 2, o, 0).start()
                self.copy(q, 2, o, 1).start()
        for q in (0, 1):
            self.wait(q, 2, 0, 0)
            self.copy(q, 2, 0, 2).start()
            self.wait(q, 2, 0, 1)
            self.copy(q, 2, 0, 3).start()
        for q in (0, 1):
            self.wait(q, 1, 0, 2)
            self.wait(q, 1, 0, 3)
            self.copy(q, 2, 2, 0).start()
            self.copy(q, 2, 2, 1).start()
        for o in (-1, 1, 2):
            for q in (0, 1):
                self.wait(q, 2, o, 0)
                self.copy(q, 2, o, 2).start()
                self.wait(q, 2, o, 1)
                self.copy(q, 2, o, 3).start()
        for o in (0, -1, 1, 2):
            for q in (0, 1):
                self.wait(q, 2, o, 2)
                self.wait(q, 2, o, 3)
        other = 1 - self.p.core
        for q, phase, o, e in self.events():
            self.across(q, phase, o, e, other).wait_recv()

    def events(self):
        for q in (0, 1):
            for e in range(4):
                yield q, 1, 0, e
            for o in (0, -1, 1, 2):
                for e in range(4):
                    yield q, 2, o, e

    def drain(self):
        for q, phase, o, e in self.events():
            self.copy(q, phase, o, e).wait_send()
            self.across(q, phase, o, e, self.p.core).wait_send()


class Scatter:
    def __init__(self, place, refs, sems):
        self.p = place
        self.gs, self.gd, self.g, self.l1, self.l2, self.l3, self.l4 = refs
        self.dsend, self.drecv, self.send, self.recv, self.send2, self.recv2 = sems
        self.half = self.g.shape[3] // 2

    def cols(self, q):
        return pl.ds(q * self.half, self.half)

    def order(self, q):
        p = self.p
        c = p.x if q == 0 else p.y
        return [p.along(c, 2), p.along(c, 1), p.along(c, -1), c]

    def block(self, q, first, second):
        return (first, second) if q == 0 else (second, first)

    def ring1(self, q, steps):
        p = self.p
        return p.along(p.y if q == 0 else p.x, steps)

    def own1(self, q):
        return self.p.y if q == 0 else self.p.x

    def pair(self, q, first, low):
        if q == 0:
            return self.g.at[first, pl.ds(low, 2), :, self.cols(q)]
        return self.g.at[pl.ds(low, 2), first, :, self.cols(q)]

    def copy1(self, q, d):
        p = self.p
        src = self.pair(q, self.ring1(q, 2), 2 * d)
        return remote(src, self.l1.at[q, d], self.send.at[0, q, d], self.recv.at[0, q, d],
                      {"mp": p.chip(1 - q, 1 if d == 0 else -1)})

    def copy2(self, q, d, k):
        p = self.p
        to = 1 if d == 0 else -1
        a, b = self.block(q, self.ring1(q, to), self.order(q)[k])
        return remote(self.g.at[a, b, :, self.cols(q)], self.l2.at[q, d, k],
                      self.send2.at[q, d, k], self.recv2.at[q, d, k], {"mp": p.chip(1 - q, to)})

    def copy3(self, q, d):
        p = self.p
        a, b = self.block(q, self.own1(q), self.order(q)[0])
        n = self.g.shape[2] // 2
        return remote(self.g.at[a, b, pl.ds(d * n, n), self.cols(q)], self.l3.at[q, d],
                      self.send.at[1, q, d], self.recv.at[1, q, d],
                      {"mp": p.chip(q, 1 if d == 0 else -1)})

    def copy4(self, q, d):
        p = self.p
        a, b = self.block(q, self.own1(q), self.order(q)[1 + d])
        return remote(self.g.at[a, b, :, self.cols(q)], self.l4.at[q, d],
                      self.send.at[2, q, d], self.recv.at[2, q, d],
                      {"mp": p.chip(q, 1 if d == 0 else -1)})

    def exchange(self, k):
        at = self.p.along(self.p.y, (2, 1, -1, 0)[k])
        return remote(self.gs.at[at], self.gd.at[at], self.dsend.at[k], self.drecv.at[k],
                      {"dp": 1 - self.p.core})

    def products(self, left, right):
        p = self.p
        per = self.g.shape[1] * self.g.shape[2]
        total = self.g.shape[3]
        step = min(512, total)

        def product(core, at, store):
            start = pl.multiple_of(core * (SIDE * per) + at * per, per)
            rows = left(pl.ds(start, per))

            def tile(n, _):
                cols = pl.ds(pl.multiple_of(n * step, step), step)
                value = lax.dot_general(
                    rows, right(cols), (((0,), (0,)), ((), ())), preferred_element_type=F32
                )
                store(at, cols, value.reshape(SIDE, self.g.shape[2], step))
                return 0

            lax.fori_loop(0, total // step, tile, 0)

        def to_other(at, cols, value):
            self.gs[at, :, :, cols] = value.astype(BF16)

        def to_own(at, cols, value):
            self.g[at, :, :, cols] = (value + self.gd[at, :, :, cols].astype(F32)).astype(BF16)

        for k in range(SIDE):
            at = p.along(p.y, (2, 1, -1, 0)[k])
            product(1 - p.core, at, to_other)
            self.exchange(k).start()
        for k in range(SIDE):
            at = p.along(p.y, (2, 1, -1, 0)[k])
            self.exchange(k).wait_recv()
            product(p.core, at, to_own)
            if k == 0:
                self.copy1(0, 0).start()
                self.copy1(0, 1).start()
        self.copy1(1, 0).start()
        self.copy1(1, 1).start()

    def add(self, index, value):
        self.g[index] = (self.g[index].astype(F32) + value.astype(F32)).astype(BF16)

    def run(self, finish):
        n = self.g.shape[2] // 2
        for d in (0, 1):
            for q in (0, 1):
                self.copy1(q, d).wait_recv()
                first = self.ring1(q, 1 if d == 0 else -1)
                for k in (0, 1):
                    a, b = self.block(q, first, 2 * d + k)
                    self.add((a, b, slice(None), self.cols(q)), self.l1[q, d, k])
                for k in range(SIDE):
                    self.copy2(q, d, k).start()
        for k in range(SIDE):
            for q in (0, 1):
                self.copy2(q, 0, k).wait_recv()
                self.copy2(q, 1, k).wait_recv()
                a, b = self.block(q, self.own1(q), self.order(q)[k])
                self.add(
                    (a, b, slice(None), self.cols(q)),
                    self.l2[q, 0, k].astype(F32) + self.l2[q, 1, k].astype(F32),
                )
                if k == 0:
                    self.copy3(q, 0).start()
                    self.copy3(q, 1).start()
                if k in (1, 2):
                    d = k - 1
                    self.copy3(q, d).wait_recv()
                    self.add((a, b, pl.ds(d * n, n), self.cols(q)), self.l3[q, d])
                    self.copy4(q, d).start()
        for q in (0, 1):
            self.copy4(q, 0).wait_recv()
            self.copy4(q, 1).wait_recv()
            a, b = self.block(q, self.own1(q), self.order(q)[3])
            finish(
                q,
                self.g[a, b, :, self.cols(q)].astype(F32)
                + self.l4[q, 0].astype(F32)
                + self.l4[q, 1].astype(F32),
            )

    def drain(self):
        for k in range(SIDE):
            self.exchange(k).wait_send()
        for q in (0, 1):
            for d in (0, 1):
                self.copy1(q, d).wait_send()
                self.copy3(q, d).wait_send()
                self.copy4(q, d).wait_send()
                for k in range(SIDE):
                    self.copy2(q, d, k).wait_send()


def step_kernel(sections, *refs):
    (
        inputs, tangents, targets, target_jac, mask, batch_order, encoder, shard, head,
        o_layer, o_head, o_loss,
        w, xin, xout, mix, cot, pin, pout, pre, thb, cin, cpin, cout, cpout, mixp, cotp,
        count_out, count_in, loss_out, loss_in, loss_sum, loss_land, head_out, head_land,
        fsend, frecv, bsend, brecv,
        gsend1, grecv1, gsend2, grecv2, dsend1, drecv1, dsend2, drecv2,
        csend, crecv, lsend, lrecv, zsend, zrecv,
        *scatter,
    ) = refs
    layer_refs, layer_sems = scatter[:7], scatter[7:13]
    head_refs, head_sems = scatter[13:20], scatter[20:26]
    n_mb, rows, width = xin.shape
    rank = cin.shape[1]
    out_width = head.shape[1]
    tile = width // PIECES
    place = Place(sections)
    s, core, first, last = place.s, place.core, place.first, place.last
    chips = SIDE * SIDE

    enter(place)
    gather = Gather(place, shard, w, (gsend1, grecv1, gsend2, grecv2, dsend1, drecv1, dsend2, drecv2))
    gather.begin()

    def totals_and_where():
        totals = 1.0 + jnp.sum(mask[...].astype(F32), axis=1, keepdims=True)
        where = lax.broadcasted_iota(jnp.int32, (n_mb, n_mb), 0) == jnp.broadcast_to(
            batch_order[...], (n_mb, n_mb)
        )
        return totals, where.astype(F32)

    def count_copy(step, receiving):
        other = lax.rem(place.mp + step, chips)
        source = lax.rem(place.mp + chips - step, chips)
        slot = source if receiving else place.mp
        return remote(count_out, count_in.at[slot], csend.at[step], crecv.at[step], {"mp": other})

    @pl.when(last)
    def _():
        totals, where = totals_and_where()
        count_out[...] = jnp.zeros_like(count_out)
        count_out[0:1, 0:n_mb] = jnp.sum(where * totals, axis=0, keepdims=True)
        count_in[place.mp] = count_out[...]
        lax.fori_loop(1, chips, lambda i, _: (count_copy(i, False).start(), 0)[1], 0)

    @pl.when(first)
    def _():
        primal = inputs[...].astype(F32)
        for m in range(n_mb):
            lhs = jnp.concatenate(
                [tangents[m], first_row(primal[m : m + 1], rows - rank).astype(BF16)], axis=0
            )
            lifted = jnp.dot(lhs, encoder[...], preferred_element_type=F32).astype(BF16)
            xin[m] = lifted
            pin[m] = lifted[rank:].astype(F32)[0:1]

    gather.run()

    def fcopy(m, j):
        cols = pl.ds(j * tile, tile)
        return remote(
            xout.at[m, pl.ds(0, rank), cols], xin.at[m, pl.ds(0, rank), cols],
            fsend.at[m, j], frecv.at[m, j], {"section": place.nxt},
        )

    def fpcopy(m):
        return remote(
            pout.at[m], pin.at[m], fsend.at[m, PIECES], frecv.at[m, PIECES], {"section": place.nxt}
        )

    def bcopy(m, j):
        cols = pl.ds(j * tile, tile)
        return remote(
            cout.at[m, :, cols], cin.at[m, :, cols],
            bsend.at[m, j], brecv.at[m, j], {"section": place.prv},
        )

    def bpcopy(m):
        return remote(
            cpout.at[m], cpin.at[m], bsend.at[m, PIECES], brecv.at[m, PIECES], {"section": place.prv}
        )

    def forward(m, _):
        @pl.when(jnp.logical_not(first))
        def _():
            for j in range(PIECES):
                fcopy(m, j).wait_recv()
            fpcopy(m).wait_recv()
            xin[m, pl.ds(rank, rows - rank), :] = first_row(pin[m], rows - rank).astype(BF16)

        for j in range(PIECES):
            cols = pl.ds(j * tile, tile)
            acc = jnp.dot(xin[m], w[:, cols], preferred_element_type=F32)
            th = jnp.tanh(acc[rank : rank + 1, :])
            slope = 1.0 - th * th
            tangent = acc[:rank, :]
            pre[m, :, cols] = tangent
            thb[m, :, cols] = th
            moved = xin[m, pl.ds(0, rank), cols].astype(F32) + slope * tangent
            xout[m, pl.ds(0, rank), cols] = moved.astype(BF16)
            primal = (pin[m, :, cols] + th).astype(BF16).astype(F32)
            pout[m, :, cols] = primal
            xout[m, pl.ds(rank, rows - rank), cols] = first_row(primal, rows - rank).astype(BF16)

            @pl.when(jnp.logical_not(last))
            def _():
                fcopy(m, j).start()

        @pl.when(jnp.logical_not(last))
        def _():
            fpcopy(m).start()

        return 0

    lax.fori_loop(0, n_mb, forward, 0)

    def loss_copy(step, receiving):
        plane = 2 * chips
        me = core * chips + place.mp
        other = lax.rem(me + step, plane)
        source = lax.rem(me + plane - step, plane)
        slot = source if receiving else me
        return remote(
            loss_out, loss_in.at[slot], lsend.at[step], lrecv.at[step],
            {"dp": other // chips, "mp": lax.rem(other, chips)},
        )

    @pl.when(last)
    def _():
        lax.fori_loop(1, chips, lambda i, _: (count_copy(i, True).wait_recv(), 0)[1], 0)
        totals, where = totals_and_where()
        counts = jnp.sum(count_in[...], axis=0)[0:1, 0:n_mb]
        inverse = 1.0 / jnp.sum(where * counts, axis=1, keepdims=True)
        row = lax.broadcasted_iota(jnp.int32, (rows, 1), 0)
        ranks = totals.astype(jnp.int32) - 1
        step = min(256, out_width)
        total = jnp.zeros((1, 1), F32)
        for n in range(out_width // step):
            cols = pl.ds(n * step, step)
            outputs = jnp.dot(
                xout[...].reshape(n_mb * rows, width), head[:, cols], preferred_element_type=F32
            )
            primal_wanted = targets[:, cols].astype(F32)
            for m in range(n_mb):
                wanted = jnp.concatenate(
                    [
                        target_jac[m, :, cols].astype(F32),
                        first_row(primal_wanted[m : m + 1], rows - rank),
                    ],
                    axis=0,
                )
                present = jnp.logical_or(row < ranks[m : m + 1], row == rank)
                scale = jnp.where(present, inverse[m : m + 1], 0.0)
                mismatch = outputs[m * rows : (m + 1) * rows] - wanted
                weighted = scale * mismatch
                total = total + jnp.sum(
                    jnp.sum(weighted * mismatch, axis=0, keepdims=True), axis=1, keepdims=True
                )
                rounded = (2.0 * weighted).astype(BF16)
                cot[m, :, cols] = rounded
                cotp[m, :, cols] = rounded[rank:].astype(F32)[0:1]
        loss_out[...] = jnp.broadcast_to(total, loss_out.shape)
        loss_in[core * chips + place.mp] = loss_out[...]
        lax.fori_loop(1, 2 * chips, lambda i, _: (loss_copy(i, False).start(), 0)[1], 0)
        for n in range(width // step):
            cols = pl.ds(n * step, step)
            grads = lax.dot_general(
                cot[...].reshape(n_mb * rows, out_width), head[cols, :], (((1,), (1,)), ((), ())),
                preferred_element_type=F32,
            ).astype(BF16)
            for m in range(n_mb):
                cin[m, :, cols] = grads[m * rows : m * rows + rank, :]
                cpin[m, :, cols] = grads[m * rows + rank : m * rows + rows, :].astype(F32)[0:1]

    def backward(m, _):
        @pl.when(jnp.logical_not(last))
        def _():
            for j in range(PIECES):
                bcopy(m, j).wait_recv()
            bpcopy(m).wait_recv()

        for j in range(PIECES):
            cols = pl.ds(j * tile, tile)
            upstream = cin[m, :, cols].astype(F32)
            th = thb[m, :, cols]
            slope = 1.0 - th * th
            mix[m, pl.ds(0, rank), cols] = (upstream * slope).astype(BF16)
            total = jnp.sum(upstream * pre[m, :, cols], axis=0, keepdims=True)
            primal = cpin[m, :, cols] * slope - 2.0 * total * th * slope
            mixp[m, :, cols] = primal
            mix[m, pl.ds(rank, rows - rank), cols] = first_row(primal, rows - rank).astype(BF16)

        @pl.when(jnp.logical_not(first))
        def _():
            for j in range(PIECES):
                cols = pl.ds(j * tile, tile)
                back = lax.dot_general(
                    mix[m], w[cols, :], (((1,), (1,)), ((), ())), preferred_element_type=F32
                )
                cout[m, :, cols] = (cin[m, :, cols].astype(F32) + back[:rank]).astype(BF16)
                cpout[m, :, cols] = (
                    (cpin[m, :, cols] + back[rank : rank + 1]).astype(BF16).astype(F32)
                )
                bcopy(m, j).start()
            bpcopy(m).start()

        return 0

    lax.fori_loop(0, n_mb, backward, 0)

    def compact(tangent, primal):
        def take(cols):
            block = tangent[:, pl.ds(0, rank), cols]
            rest = stacked_rows(lambda m: primal[m, :, cols], n_mb, 16, block.shape[2])
            return jnp.concatenate(
                [block.reshape(n_mb * rank, block.shape[2]), rest.astype(BF16)], axis=0
            )

        return take

    def section_copy(step, what):
        other = lax.rem(place.s + step, sections)
        if what == 0:
            return remote(head_out.at[other], head_land, zsend.at[0, step], zrecv.at[0], {"section": other})
        return remote(loss_sum, loss_land, zsend.at[1, step], zrecv.at[1], {"section": other})

    heads = Scatter(place, head_refs, head_sems)

    @pl.when(last)
    def _():
        heads.products(compact(xout, pout), compact(cot, cotp))

        def finish(q, value):
            per = out_width // sections
            for k in range(heads.half // per):
                head_out[q * (heads.half // per) + k] = value[:, k * per : (k + 1) * per]

        heads.run(finish)
        lax.fori_loop(1, 2 * chips, lambda i, _: (loss_copy(i, True).wait_recv(), 0)[1], 0)
        loss_sum[...] = jnp.sum(loss_in[...], axis=0)

        def spread(i, _):
            section_copy(i, 0).start()
            section_copy(i, 1).start()
            return 0

        lax.fori_loop(1, sections, spread, 0)
        o_head[...] = head_out[sections - 1]
        o_loss[...] = loss_sum[...]

    sums = Scatter(place, layer_refs, layer_sems)
    sums.products(compact(xin, pin), compact(mix, mixp))

    def finish_layer(q, value):
        o_layer[:, pl.ds(q * sums.half, sums.half)] = value

    sums.run(finish_layer)

    @pl.when(jnp.logical_not(last))
    def _():
        section_copy(1, 0).wait_recv()
        section_copy(1, 1).wait_recv()
        o_head[...] = head_land[...]
        o_loss[...] = loss_land[...]

    def drain(m, _):
        @pl.when(jnp.logical_not(last))
        def _():
            for j in range(PIECES):
                fcopy(m, j).wait_send()
            fpcopy(m).wait_send()

        @pl.when(jnp.logical_not(first))
        def _():
            for j in range(PIECES):
                bcopy(m, j).wait_send()
            bpcopy(m).wait_send()

        return 0

    lax.fori_loop(0, n_mb, drain, 0)
    gather.drain()
    sums.drain()

    @pl.when(last)
    def _():
        heads.drain()
        lax.fori_loop(1, chips, lambda i, _: (count_copy(i, False).wait_send(), 0)[1], 0)
        lax.fori_loop(1, 2 * chips, lambda i, _: (loss_copy(i, False).wait_send(), 0)[1], 0)

        def spread(i, _):
            section_copy(i, 0).wait_send()
            section_copy(i, 1).wait_send()
            return 0

        lax.fori_loop(1, sections, spread, 0)


def scatter_scratch(rows, cols):
    half = cols // 2
    dma = pltpu.SemaphoreType.DMA
    part = (SIDE, SIDE, rows, cols)
    return [
        pltpu.VMEM(part, BF16),
        pltpu.VMEM(part, BF16),
        pltpu.VMEM(part, BF16),
        pltpu.VMEM((2, 2, 2, rows, half), BF16),
        pltpu.VMEM((2, 2, SIDE, rows, half), BF16),
        pltpu.VMEM((2, 2, rows // 2, half), BF16),
        pltpu.VMEM((2, 2, rows, half), BF16),
        dma((SIDE,)), dma((SIDE,)),
        dma((3, 2, 2)), dma((3, 2, 2)),
        dma((2, 2, SIDE)), dma((2, 2, SIDE)),
    ]


def local(
    inputs, tangents, targets, target_jac, rank_mask, batch_order, encoder, layers, head_weight
):
    n_mb, rank, _ = tangents.shape
    width = layers.shape[2]
    out_width = head_weight.shape[1]
    sections = lax.axis_size("section")
    chips = SIDE * SIDE
    own = width // (2 * chips)
    per = out_width // sections
    dma = pltpu.SemaphoreType.DMA
    vmem = pl.BlockSpec(memory_space=pltpu.VMEM)
    row = pltpu.VMEM((n_mb, 1, width), F32)
    block = pltpu.VMEM((n_mb, ROWS, width), BF16)
    send = pltpu.VMEM((n_mb, rank, width), BF16)
    grad_layer, grad_head, loss = pl.pallas_call(
        functools.partial(step_kernel, sections),
        out_shape=(
            jax.ShapeDtypeStruct((own, width), F32),
            jax.ShapeDtypeStruct((own, per), F32),
            jax.ShapeDtypeStruct((8, 128), F32),
        ),
        in_specs=[vmem] * 9,
        out_specs=(vmem,) * 3,
        scratch_shapes=[
            pltpu.VMEM((width, width), BF16),
            block, block, block,
            pltpu.VMEM((n_mb, ROWS, out_width), BF16),
            row, row,
            pltpu.VMEM((n_mb, rank, width), F32),
            row, send, row, send, row, row,
            pltpu.VMEM((n_mb, 1, out_width), F32),
            pltpu.VMEM((8, 128), F32),
            pltpu.VMEM((chips, 8, 128), F32),
            pltpu.VMEM((8, 128), F32),
            pltpu.VMEM((2 * chips, 8, 128), F32),
            pltpu.VMEM((8, 128), F32),
            pltpu.VMEM((8, 128), F32),
            pltpu.VMEM((sections, own, per), F32),
            pltpu.VMEM((own, per), F32),
            dma((n_mb, PIECES + 1)), dma((n_mb, PIECES + 1)),
            dma((n_mb, PIECES + 1)), dma((n_mb, PIECES + 1)),
            dma((2, 4)), dma((2, 4)), dma((2, SIDE, 4)), dma((2, SIDE, 4)),
            dma((2, 4)), dma((2, 4)), dma((2, SIDE, 4)), dma((2, SIDE, 4)),
            dma((chips,)), dma((chips,)),
            dma((2 * chips,)), dma((2 * chips,)),
            dma((2, sections)), dma((2,)),
            *scatter_scratch(own, width),
            *scatter_scratch(own, out_width),
        ],
        compiler_params=pltpu.CompilerParams(
            collective_id=0, has_side_effects=True, vmem_limit_bytes=67043328
        ),
        name="step",
    )(
        inputs, tangents, targets, target_jac, rank_mask, batch_order, encoder, layers[0],
        head_weight,
    )
    loss_value = loss[0, 0] / (lax.axis_size("dp") * n_mb * out_width)
    return grad_layer[None], grad_head, loss_value


def solution(mesh):
    in_specs = (
        P(("dp", "mp"), None),
        P(("dp", "mp"), None, None),
        P(("dp", "mp"), None),
        P(("dp", "mp"), None, None),
        P(("dp", "mp"), None),
        P(("dp", "mp"), None),
        P(),
        P("section", "mp", None),
        P(),
    )
    out_specs = (P("section", ("dp", "mp"), None), P(("dp", "mp"), "section"), P())
    return jax.shard_map(local, mesh=mesh, in_specs=in_specs, out_specs=out_specs, check_vma=False)
```

```python
import functools

import jax
import jax.numpy as jnp
from jax import lax
from jax.experimental import pallas as pl
from jax.experimental.pallas import tpu as pltpu
from jax.sharding import PartitionSpec as P

SIDE = 4
ROWS = 48
PIECES = 4
MESH = pl.DeviceIdType.MESH
BF16, F32 = jnp.bfloat16, jnp.float32


def first_row(row, height):
    rows = lax.broadcasted_iota(jnp.int32, (height, row.shape[1]), 0)
    return jnp.where(rows == 0, jnp.broadcast_to(row, (height, row.shape[1])), 0.0)


def stacked_rows(get_row, count, height, width):
    rows = lax.broadcasted_iota(jnp.int32, (height, width), 0)
    block = jnp.zeros((height, width), F32)
    for m in range(count):
        block = jnp.where(rows == m, jnp.broadcast_to(get_row(m), (height, width)), block)
    return block


class Place:
    def __init__(self, sections):
        self.sections = sections
        self.core = lax.axis_index("dp")
        self.s = lax.axis_index("section")
        self.mp = lax.axis_index("mp")
        self.y = self.mp // SIDE
        self.x = lax.rem(self.mp, SIDE)
        self.first = self.s == 0
        self.last = self.s == sections - 1
        self.nxt = lax.rem(self.s + 1, sections)
        self.prv = lax.rem(self.s + sections - 1, sections)

    def along(self, coordinate, steps):
        return lax.rem(coordinate + steps + SIDE, SIDE)

    def chip(self, axis, steps):
        if axis == 0:
            return self.y * SIDE + self.along(self.x, steps)
        return self.along(self.y, steps) * SIDE + self.x


def remote(src, dst, send, recv, device_id):
    return pltpu.make_async_remote_copy(
        src_ref=src, dst_ref=dst, send_sem=send, recv_sem=recv,
        device_id=device_id, device_id_type=MESH,
    )


def enter(place):
    barrier = pltpu.get_barrier_semaphore()
    plane = 2 * SIDE * SIDE
    me = place.core * (SIDE * SIDE) + place.mp

    def tell_plane(step, _):
        other = lax.rem(me + step, plane)
        pl.semaphore_signal(
            barrier, inc=1,
            device_id={"dp": other // (SIDE * SIDE), "mp": lax.rem(other, SIDE * SIDE)},
            device_id_type=MESH,
        )
        return 0

    def tell_column(step, _):
        other = lax.rem(place.s + step, place.sections)
        pl.semaphore_signal(barrier, inc=1, device_id={"section": other}, device_id_type=MESH)
        return 0

    lax.fori_loop(1, plane, tell_plane, 0)
    lax.fori_loop(1, place.sections, tell_column, 0)
    pl.semaphore_wait(barrier, plane - 1 + place.sections - 1)


class Gather:
    def __init__(self, place, shard, w, sems):
        self.p, self.shard, self.w = place, shard, w
        self.sent, self.recv1, self.recv2, self.dsent, self.dgot = sems
        self.depth = shard.shape[0]
        self.piece = self.depth // 4

    def rows(self, q, core, step1, step2, half):
        p = self.p
        dx, dy = (step1, step2) if q == 0 else (step2, step1)
        chip = p.along(p.y, dy) * SIDE + p.along(p.x, dx)
        start = chip * self.depth + core * (2 * self.piece) + q * self.piece
        length = self.piece
        if half is not None:
            length = self.piece // 2
            start = start + half * length
        return pl.ds(pl.multiple_of(start, length), length)

    def copy(self, q, phase, o, e):
        p = self.p
        axis = q if phase == 1 else 1 - q
        to = 1 if e in (0, 2) else -1
        back = {0: 0, 1: 0, 2: -1, 3: 1}[e]
        half = {0: None, 1: None, 2: 0, 3: 1}[e]
        step1, step2 = (back, 0) if phase == 1 else (o, back)
        dst = self.w.at[self.rows(q, p.core, step1, step2, half)]
        src = dst
        if step1 == 0 and step2 == 0:
            src = self.shard.at[pl.ds(pl.multiple_of(p.core * (2 * self.piece) + q * self.piece, self.piece), self.piece)]
        return remote(src, dst, self.sent, self.recv(phase, q, o, e), {"mp": p.chip(axis, to)})

    def recv(self, phase, q, o, e):
        return self.recv1.at[q, e] if phase == 1 else self.recv2.at[q, o % SIDE, e]

    def arrived(self, q, phase, o, e):
        p = self.p
        away = {0: -1, 1: 1, 2: -2, 3: 2}[e]
        half = {0: None, 1: None, 2: 0, 3: 1}[e]
        step1, step2 = (away, 0) if phase == 1 else (o, away)
        return self.p, q, step1, step2, half

    def wait(self, q, phase, o, e):
        p, q, step1, step2, half = self.arrived(q, phase, o, e)
        dst = self.w.at[self.rows(q, p.core, step1, step2, half)]
        remote(dst, dst, self.sent, self.recv(phase, q, o, e), {"mp": p.chip(0, 1)}).wait_recv()
        remote(dst, dst, self.dsent, self.dgot, {"dp": 1 - p.core}).start()

    def all_of(self, send, recv):
        ref = self.w.at[pl.ds(0, (SIDE * SIDE - 1) * 2 * self.piece)]
        return remote(ref, ref, send, recv, {"dp": 1 - self.p.core})

    def begin(self):
        for q in (0, 1):
            self.copy(q, 1, 0, 0).start()
            self.copy(q, 1, 0, 1).start()
        for q in (0, 1):
            self.copy(q, 2, 0, 0).start()
            self.copy(q, 2, 0, 1).start()
        p = self.p
        self.w[pl.ds(pl.multiple_of(p.mp * self.depth, self.depth), self.depth), :] = self.shard[...]

    def run(self, meanwhile):
        for q in (0, 1):
            self.wait(q, 1, 0, 0)
            self.copy(q, 1, 0, 2).start()
            self.wait(q, 1, 0, 1)
            self.copy(q, 1, 0, 3).start()
        for q in (0, 1):
            for o in (-1, 1):
                self.copy(q, 2, o, 0).start()
                self.copy(q, 2, o, 1).start()
        meanwhile()
        for q in (0, 1):
            self.wait(q, 2, 0, 0)
            self.copy(q, 2, 0, 2).start()
            self.wait(q, 2, 0, 1)
            self.copy(q, 2, 0, 3).start()
        for q in (0, 1):
            self.wait(q, 1, 0, 2)
            self.wait(q, 1, 0, 3)
            self.copy(q, 2, 2, 0).start()
            self.copy(q, 2, 2, 1).start()
        for o in (-1, 1, 2):
            for q in (0, 1):
                self.wait(q, 2, o, 0)
                self.copy(q, 2, o, 2).start()
                self.wait(q, 2, o, 1)
                self.copy(q, 2, o, 3).start()
        for o in (0, -1, 1, 2):
            for q in (0, 1):
                self.wait(q, 2, o, 2)
                self.wait(q, 2, o, 3)
        self.all_of(self.dsent, self.dgot).wait_recv()

    def drain(self):
        self.all_of(self.sent, self.dgot).wait_send()
        self.all_of(self.dsent, self.dgot).wait_send()


class Scatter:
    def __init__(self, place, refs, sems):
        self.p = place
        self.gs, self.gd, self.g, self.l1, self.l2, self.l3, self.l4, self.turned = refs
        self.sent, self.drecv, self.recv, self.recv2 = sems
        self.half = self.g.shape[3] // 2

    def cols(self, q):
        return pl.ds(q * self.half, self.half)

    def order(self, q):
        p = self.p
        c = p.x if q == 0 else p.y
        return [p.along(c, 2), p.along(c, 1), p.along(c, -1), c]

    def block(self, q, first, second):
        return (first, second) if q == 0 else (second, first)

    def ring1(self, q, steps):
        p = self.p
        return p.along(p.y if q == 0 else p.x, steps)

    def own1(self, q):
        return self.p.y if q == 0 else self.p.x

    def pair(self, q, first, low):
        if q == 0:
            return self.g.at[first, pl.ds(low, 2), :, self.cols(q)]
        return self.g.at[pl.ds(low, 2), first, :, self.cols(q)]

    def copy1(self, q, d):
        p = self.p
        src = self.pair(q, self.ring1(q, 2), 2 * d)
        return remote(src, self.l1.at[q, d], self.sent.at[1], self.recv.at[0, q, d],
                      {"mp": p.chip(1 - q, 1 if d == 0 else -1)})

    def copy2(self, q, d, k):
        p = self.p
        to = 1 if d == 0 else -1
        a, b = self.block(q, self.ring1(q, to), self.order(q)[k])
        return remote(self.g.at[a, b, :, self.cols(q)], self.l2.at[q, d, k],
                      self.sent.at[2], self.recv2.at[q, d, k], {"mp": p.chip(1 - q, to)})

    def copy3(self, q, d):
        p = self.p
        a, b = self.block(q, self.own1(q), self.order(q)[0])
        n = self.g.shape[2] // 2
        return remote(self.g.at[a, b, pl.ds(d * n, n), self.cols(q)], self.l3.at[q, d],
                      self.sent.at[3], self.recv.at[1, q, d],
                      {"mp": p.chip(q, 1 if d == 0 else -1)})

    def copy4(self, q, d):
        p = self.p
        a, b = self.block(q, self.own1(q), self.order(q)[1 + d])
        return remote(self.g.at[a, b, :, self.cols(q)], self.l4.at[q, d],
                      self.sent.at[4], self.recv.at[2, q, d],
                      {"mp": p.chip(q, 1 if d == 0 else -1)})

    def exchange(self, k):
        at = self.p.along(self.p.y, (2, 1, -1, 0)[k])
        return remote(self.gs.at[at], self.gd.at[at], self.sent.at[0], self.drecv.at[k],
                      {"dp": 1 - self.p.core})

    def products(self, left, right):
        p = self.p
        per = self.g.shape[1] * self.g.shape[2]
        total = self.g.shape[3]
        step = min(512, total)

        def product(core, at, store):
            start = pl.multiple_of(core * (SIDE * per) + at * per, per)
            self.turned[...] = left(pl.ds(start, per)).T

            def tile(n, _):
                cols = pl.ds(pl.multiple_of(n * step, step), step)
                value = jnp.dot(self.turned[...], right(cols), preferred_element_type=F32)
                store(at, cols, value.reshape(SIDE, self.g.shape[2], step))
                return 0

            lax.fori_loop(0, total // step, tile, 0)

        def to_other(at, cols, value):
            self.gs[at, :, :, cols] = value.astype(BF16)

        def to_own(at, cols, value):
            self.g[at, :, :, cols] = (value + self.gd[at, :, :, cols].astype(F32)).astype(BF16)

        for k in range(SIDE):
            at = p.along(p.y, (2, 1, -1, 0)[k])
            product(1 - p.core, at, to_other)
            self.exchange(k).start()
        for k in range(SIDE):
            at = p.along(p.y, (2, 1, -1, 0)[k])
            self.exchange(k).wait_recv()
            product(p.core, at, to_own)
            if k == 0:
                self.copy1(0, 0).start()
                self.copy1(0, 1).start()
        self.copy1(1, 0).start()
        self.copy1(1, 1).start()

    def add(self, index, value):
        self.g[index] = (self.g[index].astype(F32) + value.astype(F32)).astype(BF16)

    def run(self, finish):
        n = self.g.shape[2] // 2
        for d in (0, 1):
            for q in (0, 1):
                self.copy1(q, d).wait_recv()
                first = self.ring1(q, 1 if d == 0 else -1)
                for k in (0, 1):
                    a, b = self.block(q, first, 2 * d + k)
                    self.add((a, b, slice(None), self.cols(q)), self.l1[q, d, k])
                for k in range(SIDE):
                    self.copy2(q, d, k).start()
        for k in range(SIDE):
            for q in (0, 1):
                self.copy2(q, 0, k).wait_recv()
                self.copy2(q, 1, k).wait_recv()
                a, b = self.block(q, self.own1(q), self.order(q)[k])
                self.add(
                    (a, b, slice(None), self.cols(q)),
                    self.l2[q, 0, k].astype(F32) + self.l2[q, 1, k].astype(F32),
                )
                if k == 0:
                    self.copy3(q, 0).start()
                    self.copy3(q, 1).start()
                if k in (1, 2):
                    d = k - 1
                    self.copy3(q, d).wait_recv()
                    self.add((a, b, pl.ds(d * n, n), self.cols(q)), self.l3[q, d])
                    self.copy4(q, d).start()
        for q in (0, 1):
            self.copy4(q, 0).wait_recv()
            self.copy4(q, 1).wait_recv()
            a, b = self.block(q, self.own1(q), self.order(q)[3])
            finish(
                q,
                self.g[a, b, :, self.cols(q)].astype(F32)
                + self.l4[q, 0].astype(F32)
                + self.l4[q, 1].astype(F32),
            )

    def drain(self):
        for n, ref in enumerate((self.gd, self.l1, self.l2, self.l3, self.l4)):
            remote(ref, ref, self.sent.at[n], self.drecv.at[0], {"dp": 1 - self.p.core}).wait_send()


def step_kernel(sections, loss_scale, *refs):
    (
        h_inputs, h_tangents, h_targets, h_target_jac, mask, batch_order, h_encoder, h_shard, h_head,
        o_layer, o_head, o_loss,
        inputs, tangents, targets, target_jac, encoder, shard, head,
        w, wt, xin, xout, mix, cot, pin, pout, pre, thb, cin, cpin, cout, cpout, mixp, cotp,
        count_out, count_in, loss_out, loss_in, loss_sum, loss_land, head_out, head_land,
        loads, relayed, frecv, brecv,
        gsent, grecv1, grecv2, dsent, dgot,
        csend, crecv, lsend, lrecv, zsend, zrecv,
        *scatter,
    ) = refs
    layer_refs, layer_sems = scatter[:8], scatter[8:12]
    head_refs, head_sems = scatter[12:20], scatter[20:24]
    n_mb, rows, width = xin.shape
    rank = cin.shape[1]
    out_width = head.shape[1]
    tile = width // PIECES
    place = Place(sections)
    s, core, first, last = place.s, place.core, place.first, place.last
    chips = SIDE * SIDE

    def load(n):
        pairs = (
            (h_shard, shard), (h_inputs, inputs), (h_tangents, tangents), (h_encoder, encoder),
            (h_targets, targets), (h_target_jac, target_jac), (h_head, head),
        )
        return pltpu.make_async_copy(pairs[n][0], pairs[n][1], loads.at[n])

    for n in range(7):
        load(n).start()
    enter(place)
    load(0).wait()
    gather = Gather(place, shard, w, (gsent, grecv1, grecv2, dsent, dgot))
    gather.begin()

    def totals_and_where():
        totals = 1.0 + jnp.sum(mask[...].astype(F32), axis=1, keepdims=True)
        where = lax.broadcasted_iota(jnp.int32, (n_mb, n_mb), 0) == jnp.broadcast_to(
            batch_order[...], (n_mb, n_mb)
        )
        return totals, where.astype(F32)

    def count_copy(step):
        other = lax.rem(place.mp + step, chips)
        slot = place.mp
        return remote(count_out, count_in.at[slot], csend.at[0], crecv.at[0], {"mp": other})

    @pl.when(last)
    def _():
        totals, where = totals_and_where()
        count_out[...] = jnp.zeros_like(count_out)
        count_out[0:1, 0:n_mb] = jnp.sum(where * totals, axis=0, keepdims=True)
        count_in[place.mp] = count_out[...]
        lax.fori_loop(1, chips, lambda i, _: (count_copy(i).start(), 0)[1], 0)

    def all_counts():
        ref = count_in.at[pl.ds(0, chips - 1)]
        return remote(ref, ref, csend.at[0], crecv.at[0], {"dp": 1 - core})

    def all_losses():
        ref = loss_in.at[pl.ds(0, 2 * chips - 1)]
        return remote(ref, ref, lsend.at[0], lrecv.at[0], {"dp": 1 - core})

    def encode():
        for n in range(1, 7):
            load(n).wait()

        @pl.when(first)
        def _():
            primal = inputs[...].astype(F32)
            for m in range(n_mb):
                lhs = jnp.concatenate(
                    [tangents[m], first_row(primal[m : m + 1], rows - rank).astype(BF16)], axis=0
                )
                lifted = jnp.dot(lhs, encoder[...], preferred_element_type=F32).astype(BF16)
                xin[m] = lifted
                pin[m] = lifted[rank:].astype(F32)[0:1]

    gather.run(encode)

    def turn_layer():
        step = min(512, width)
        count = width // step

        def turn(n, _):
            a = pl.ds(pl.multiple_of((n // count) * step, step), step)
            b = pl.ds(pl.multiple_of(lax.rem(n, count) * step, step), step)
            wt[b, a] = w[a, b].T
            return 0

        lax.fori_loop(0, count * count, turn, 0)

    late = s >= sections // 2

    @pl.when(late)
    def _():
        turn_layer()

    def fcopy(m, j):
        cols = pl.ds(j * tile, tile)
        return remote(
            xout.at[m, pl.ds(0, rank), cols], xin.at[m, pl.ds(0, rank), cols],
            relayed.at[0], frecv.at[m, 0], {"section": place.nxt},
        )

    def fpcopy(m):
        return remote(
            pout.at[m], pin.at[m], relayed.at[1], frecv.at[m, 1], {"section": place.nxt}
        )

    def bcopy(m, j):
        cols = pl.ds(j * tile, tile)
        return remote(
            cout.at[m, :, cols], cin.at[m, :, cols],
            relayed.at[2], brecv.at[m, 0], {"section": place.prv},
        )

    def bpcopy(m):
        return remote(
            cpout.at[m], cpin.at[m], relayed.at[3], brecv.at[m, 1], {"section": place.prv}
        )

    def forward(m, _):
        @pl.when(jnp.logical_not(first))
        def _():
            ref = xin.at[m, pl.ds(0, rank)]
            remote(ref, ref, relayed.at[0], frecv.at[m, 0], {"section": place.nxt}).wait_recv()
            fpcopy(m).wait_recv()
            xin[m, pl.ds(rank, rows - rank), :] = first_row(pin[m], rows - rank).astype(BF16)

        for j in range(PIECES):
            cols = pl.ds(j * tile, tile)
            acc = jnp.dot(xin[m], w[:, cols], preferred_element_type=F32)
            th = jnp.tanh(acc[rank : rank + 1, :])
            slope = 1.0 - th * th
            tangent = acc[:rank, :]
            pre[m, :, cols] = tangent
            thb[m, :, cols] = th
            moved = xin[m, pl.ds(0, rank), cols].astype(F32) + slope * tangent
            xout[m, pl.ds(0, rank), cols] = moved.astype(BF16)
            primal = (pin[m, :, cols] + th).astype(BF16).astype(F32)
            pout[m, :, cols] = primal
            xout[m, pl.ds(rank, rows - rank), cols] = first_row(primal, rows - rank).astype(BF16)

            @pl.when(jnp.logical_not(last))
            def _():
                fcopy(m, j).start()

        @pl.when(jnp.logical_not(last))
        def _():
            fpcopy(m).start()

        return 0

    lax.fori_loop(0, n_mb, forward, 0)

    @pl.when(jnp.logical_and(jnp.logical_not(late), jnp.logical_not(first)))
    def _():
        turn_layer()

    def loss_copy(step):
        plane = 2 * chips
        me = core * chips + place.mp
        other = lax.rem(me + step, plane)
        slot = me
        return remote(
            loss_out, loss_in.at[slot], lsend.at[0], lrecv.at[0],
            {"dp": other // chips, "mp": lax.rem(other, chips)},
        )

    @pl.when(last)
    def _():
        all_counts().wait_recv()
        totals, where = totals_and_where()
        counts = jnp.sum(count_in[...], axis=0)[0:1, 0:n_mb]
        inverse = 1.0 / jnp.sum(where * counts, axis=1, keepdims=True)
        row = lax.broadcasted_iota(jnp.int32, (rows, 1), 0)
        ranks = totals.astype(jnp.int32) - 1
        step = min(256, out_width)
        total = jnp.zeros((1, 1), F32)
        for n in range(out_width // step):
            cols = pl.ds(n * step, step)
            outputs = jnp.dot(
                xout[...].reshape(n_mb * rows, width), head[:, cols], preferred_element_type=F32
            )
            primal_wanted = targets[:, cols].astype(F32)
            for m in range(n_mb):
                wanted = jnp.concatenate(
                    [
                        target_jac[m, :, cols].astype(F32),
                        first_row(primal_wanted[m : m + 1], rows - rank),
                    ],
                    axis=0,
                )
                present = jnp.logical_or(row < ranks[m : m + 1], row == rank)
                scale = jnp.where(present, inverse[m : m + 1], 0.0)
                mismatch = outputs[m * rows : (m + 1) * rows] - wanted
                weighted = scale * mismatch
                total = total + jnp.sum(
                    jnp.sum(weighted * mismatch, axis=0, keepdims=True), axis=1, keepdims=True
                )
                rounded = (2.0 * weighted).astype(BF16)
                cot[m, :, cols] = rounded
                cotp[m, :, cols] = rounded[rank:].astype(F32)[0:1]
        loss_out[...] = jnp.broadcast_to(total, loss_out.shape)
        loss_in[core * chips + place.mp] = loss_out[...]
        lax.fori_loop(1, 2 * chips, lambda i, _: (loss_copy(i).start(), 0)[1], 0)
        for n in range(width // step):
            cols = pl.ds(n * step, step)
            grads = lax.dot_general(
                cot[...].reshape(n_mb * rows, out_width), head[cols, :], (((1,), (1,)), ((), ())),
                preferred_element_type=F32,
            ).astype(BF16)
            for m in range(n_mb):
                cin[m, :, cols] = grads[m * rows : m * rows + rank, :]
                cpin[m, :, cols] = grads[m * rows + rank : m * rows + rows, :].astype(F32)[0:1]

    def backward(m, _):
        @pl.when(jnp.logical_not(last))
        def _():
            ref = cin.at[m]
            remote(ref, ref, relayed.at[2], brecv.at[m, 0], {"section": place.prv}).wait_recv()
            bpcopy(m).wait_recv()

        for j in range(PIECES):
            cols = pl.ds(j * tile, tile)
            upstream = cin[m, :, cols].astype(F32)
            th = thb[m, :, cols]
            slope = 1.0 - th * th
            mix[m, pl.ds(0, rank), cols] = (upstream * slope).astype(BF16)
            total = jnp.sum(upstream * pre[m, :, cols], axis=0, keepdims=True)
            primal = cpin[m, :, cols] * slope - 2.0 * total * th * slope
            mixp[m, :, cols] = primal
            mix[m, pl.ds(rank, rows - rank), cols] = first_row(primal, rows - rank).astype(BF16)

        @pl.when(jnp.logical_not(first))
        def _():
            for j in range(PIECES):
                cols = pl.ds(j * tile, tile)
                back = jnp.dot(mix[m], wt[:, cols], preferred_element_type=F32)
                cout[m, :, cols] = (cin[m, :, cols].astype(F32) + back[:rank]).astype(BF16)
                cpout[m, :, cols] = (
                    (cpin[m, :, cols] + back[rank : rank + 1]).astype(BF16).astype(F32)
                )
                bcopy(m, j).start()
            bpcopy(m).start()

        return 0

    lax.fori_loop(0, n_mb, backward, 0)

    def compact(tangent, primal):
        def take(cols):
            block = tangent[:, pl.ds(0, rank), cols]
            rest = stacked_rows(lambda m: primal[m, :, cols], n_mb, 16, block.shape[2])
            return jnp.concatenate(
                [block.reshape(n_mb * rank, block.shape[2]), rest.astype(BF16)], axis=0
            )

        return take

    def section_copy(step, what):
        other = lax.rem(place.s + step, sections)
        if what == 0:
            return remote(head_out.at[other], head_land, zsend.at[0], zrecv.at[0], {"section": other})
        return remote(loss_sum, loss_land, zsend.at[1], zrecv.at[1], {"section": other})

    heads = Scatter(place, head_refs, head_sems)

    @pl.when(last)
    def _():
        heads.products(compact(xout, pout), compact(cot, cotp))

        def finish(q, value):
            per = out_width // sections
            for k in range(heads.half // per):
                head_out[q * (heads.half // per) + k] = value[:, k * per : (k + 1) * per]

        heads.run(finish)
        all_losses().wait_recv()
        loss_sum[...] = jnp.sum(loss_in[...], axis=0) * loss_scale

        def spread(i, _):
            section_copy(i, 0).start()
            section_copy(i, 1).start()
            return 0

        lax.fori_loop(1, sections, spread, 0)
        o_head[...] = head_out[sections - 1]
        o_loss[...] = loss_sum[0:1, 0:1]

    sums = Scatter(place, layer_refs, layer_sems)
    sums.products(compact(xin, pin), compact(mix, mixp))

    def finish_layer(q, value):
        o_layer[:, pl.ds(q * sums.half, sums.half)] = value

    sums.run(finish_layer)

    @pl.when(jnp.logical_not(last))
    def _():
        section_copy(1, 0).wait_recv()
        section_copy(1, 1).wait_recv()
        o_head[...] = head_land[...]
        o_loss[...] = loss_land[0:1, 0:1]

    def relays_left(ref, n):
        remote(ref, ref, relayed.at[n], frecv.at[0, 0], {"section": place.nxt}).wait_send()

    @pl.when(jnp.logical_not(last))
    def _():
        relays_left(cin, 0)
        relays_left(pout, 1)

    @pl.when(jnp.logical_not(first))
    def _():
        relays_left(cout, 2)
        relays_left(cpout, 3)

    gather.drain()
    sums.drain()

    @pl.when(last)
    def _():
        heads.drain()
        all_counts().wait_send()
        all_losses().wait_send()
        for ref, n in ((head_out, 0), (loss_in, 1)):
            ref = ref.at[pl.ds(0, sections - 1)]
            remote(ref, ref, zsend.at[n], zrecv.at[n], {"section": place.nxt}).wait_send()


def scatter_scratch(rows, cols, depth):
    half = cols // 2
    dma = pltpu.SemaphoreType.DMA
    part = (SIDE, SIDE, rows, cols)
    return [
        pltpu.VMEM(part, BF16),
        pltpu.VMEM(part, BF16),
        pltpu.VMEM(part, BF16),
        pltpu.VMEM((2, 2, 2, rows, half), BF16),
        pltpu.VMEM((2, 2, SIDE, rows, half), BF16),
        pltpu.VMEM((2, 2, rows // 2, half), BF16),
        pltpu.VMEM((2, 2, rows, half), BF16),
        pltpu.VMEM((SIDE * rows, depth), BF16),
        dma((5,)), dma((SIDE,)), dma((3, 2, 2)), dma((2, 2, SIDE)),
    ]


def local(
    inputs, tangents, targets, target_jac, rank_mask, batch_order, encoder, layers, head_weight
):
    n_mb, rank, _ = tangents.shape
    width = layers.shape[2]
    out_width = head_weight.shape[1]
    sections = lax.axis_size("section")
    chips = SIDE * SIDE
    own = width // (2 * chips)
    per = out_width // sections
    dma = pltpu.SemaphoreType.DMA
    vmem = pl.BlockSpec(memory_space=pltpu.VMEM)
    hbm = pl.BlockSpec(memory_space=pl.ANY)
    like = lambda a: pltpu.VMEM(a.shape, a.dtype)
    row = pltpu.VMEM((n_mb, 1, width), F32)
    block = pltpu.VMEM((n_mb, ROWS, width), BF16)
    send = pltpu.VMEM((n_mb, rank, width), BF16)
    grad_layer, grad_head, loss = pl.pallas_call(
        functools.partial(step_kernel, sections, 1.0 / (lax.axis_size("dp") * n_mb * out_width)),
        out_shape=(
            jax.ShapeDtypeStruct((own, width), F32),
            jax.ShapeDtypeStruct((own, per), F32),
            jax.ShapeDtypeStruct((1, 1), F32),
        ),
        in_specs=[hbm] * 4 + [vmem] * 2 + [hbm] * 3,
        out_specs=(vmem,) * 3,
        scratch_shapes=[
            like(inputs), like(tangents), like(targets), like(target_jac), like(encoder),
            like(layers[0]), like(head_weight),
            pltpu.VMEM((width, width), BF16),
            pltpu.VMEM((width, width), BF16),
            block, block, block,
            pltpu.VMEM((n_mb, ROWS, out_width), BF16),
            row, row,
            pltpu.VMEM((n_mb, rank, width), F32),
            row, send, row, send, row, row,
            pltpu.VMEM((n_mb, 1, out_width), F32),
            pltpu.VMEM((8, 128), F32),
            pltpu.VMEM((chips, 8, 128), F32),
            pltpu.VMEM((8, 128), F32),
            pltpu.VMEM((2 * chips, 8, 128), F32),
            pltpu.VMEM((8, 128), F32),
            pltpu.VMEM((8, 128), F32),
            pltpu.VMEM((sections, own, per), F32),
            pltpu.VMEM((own, per), F32),
            dma((7,)), dma((4,)), dma((n_mb, 2)), dma((n_mb, 2)),
            dma, dma((2, 4)), dma((2, SIDE, 4)), dma, dma,
            dma((1,)), dma((1,)), dma((1,)), dma((1,)), dma((2,)), dma((2,)),
            *scatter_scratch(own, width, n_mb * rank + 16),
            *scatter_scratch(own, out_width, n_mb * rank + 16),
        ],
        compiler_params=pltpu.CompilerParams(
            collective_id=0, has_side_effects=True, vmem_limit_bytes=67043328
        ),
        name="step",
    )(
        inputs, tangents, targets, target_jac, rank_mask, batch_order, encoder, layers[0],
        head_weight,
    )
    return grad_layer[None], grad_head, loss.reshape(())


def solution(mesh):
    in_specs = (
        P(("dp", "mp"), None),
        P(("dp", "mp"), None, None),
        P(("dp", "mp"), None),
        P(("dp", "mp"), None, None),
        P(("dp", "mp"), None),
        P(("dp", "mp"), None),
        P(),
        P("section", "mp", None),
        P(),
    )
    out_specs = (P("section", ("dp", "mp"), None), P(("dp", "mp"), "section"), P())
    return jax.shard_map(local, mesh=mesh, in_specs=in_specs, out_specs=out_specs, check_vma=False)
```

```python
import functools

import jax
import jax.numpy as jnp
from jax import lax
from jax.experimental import pallas as pl
from jax.experimental.pallas import tpu as pltpu
from jax.sharding import PartitionSpec as P

SIDE = 4
ROWS = 48
PIECES = 4
MESH = pl.DeviceIdType.MESH
BF16, F32 = jnp.bfloat16, jnp.float32


def first_row(row, height):
    rows = lax.broadcasted_iota(jnp.int32, (height, row.shape[1]), 0)
    return jnp.where(rows == 0, jnp.broadcast_to(row, (height, row.shape[1])), 0.0)


def stacked_rows(get_row, count, height, width):
    rows = lax.broadcasted_iota(jnp.int32, (height, width), 0)
    block = jnp.zeros((height, width), F32)
    for m in range(count):
        block = jnp.where(rows == m, jnp.broadcast_to(get_row(m), (height, width)), block)
    return block


class Place:
    def __init__(self, sections):
        self.sections = sections
        self.core = lax.axis_index("dp")
        self.s = lax.axis_index("section")
        self.mp = lax.axis_index("mp")
        self.y = self.mp // SIDE
        self.x = lax.rem(self.mp, SIDE)
        self.first = self.s == 0
        self.last = self.s == sections - 1
        self.nxt = lax.rem(self.s + 1, sections)
        self.prv = lax.rem(self.s + sections - 1, sections)

    def along(self, coordinate, steps):
        return lax.rem(coordinate + steps + SIDE, SIDE)

    def chip(self, axis, steps):
        if axis == 0:
            return self.y * SIDE + self.along(self.x, steps)
        return self.along(self.y, steps) * SIDE + self.x


def remote(src, dst, send, recv, device_id):
    return pltpu.make_async_remote_copy(
        src_ref=src, dst_ref=dst, send_sem=send, recv_sem=recv,
        device_id=device_id, device_id_type=MESH,
    )


def neighbours(place):
    for axis in (0, 1):
        for steps in (1, -1):
            yield {"mp": place.chip(axis, steps)}
    yield {"dp": 1 - place.core}
    yield {"section": place.nxt}
    yield {"section": place.prv}


def knock(place):
    barrier = pltpu.get_barrier_semaphore()
    for device in neighbours(place):
        pl.semaphore_signal(barrier, inc=1, device_id=device, device_id_type=MESH)


def enter():
    pl.semaphore_wait(pltpu.get_barrier_semaphore(), 7)


class Gather:
    def __init__(self, place, shard, w, sems):
        self.p, self.shard, self.w = place, shard, w
        self.sent, self.recv1, self.recv2, self.dsent, self.dgot = sems
        self.depth = shard.shape[0]
        self.piece = self.depth // 4

    def rows(self, q, core, step1, step2, half):
        p = self.p
        dx, dy = (step1, step2) if q == 0 else (step2, step1)
        chip = p.along(p.y, dy) * SIDE + p.along(p.x, dx)
        start = chip * self.depth + core * (2 * self.piece) + q * self.piece
        length = self.piece
        if half is not None:
            length = self.piece // 2
            start = start + half * length
        return pl.ds(pl.multiple_of(start, length), length)

    def copy(self, q, phase, o, e):
        p = self.p
        axis = q if phase == 1 else 1 - q
        to = 1 if e in (0, 2) else -1
        back = {0: 0, 1: 0, 2: -1, 3: 1}[e]
        half = {0: None, 1: None, 2: 0, 3: 1}[e]
        step1, step2 = (back, 0) if phase == 1 else (o, back)
        dst = self.w.at[self.rows(q, p.core, step1, step2, half)]
        src = dst
        if step1 == 0 and step2 == 0:
            src = self.shard.at[pl.ds(pl.multiple_of(p.core * (2 * self.piece) + q * self.piece, self.piece), self.piece)]
        return remote(src, dst, self.sent, self.recv(phase, q, o, e), {"mp": p.chip(axis, to)})

    def recv(self, phase, q, o, e):
        return self.recv1.at[q, e] if phase == 1 else self.recv2.at[q, o % SIDE, e]

    def arrived(self, q, phase, o, e):
        p = self.p
        away = {0: -1, 1: 1, 2: -2, 3: 2}[e]
        half = {0: None, 1: None, 2: 0, 3: 1}[e]
        step1, step2 = (away, 0) if phase == 1 else (o, away)
        return self.p, q, step1, step2, half

    def wait(self, q, phase, o, e):
        p, q, step1, step2, half = self.arrived(q, phase, o, e)
        dst = self.w.at[self.rows(q, p.core, step1, step2, half)]
        remote(dst, dst, self.sent, self.recv(phase, q, o, e), {"mp": p.chip(0, 1)}).wait_recv()
        remote(dst, dst, self.dsent, self.dgot, {"dp": 1 - p.core}).start()

    def all_of(self, send, recv):
        ref = self.w.at[pl.ds(0, (SIDE * SIDE - 1) * 2 * self.piece)]
        return remote(ref, ref, send, recv, {"dp": 1 - self.p.core})

    def begin(self):
        for q in (0, 1):
            self.copy(q, 1, 0, 0).start()
            self.copy(q, 1, 0, 1).start()
        for q in (0, 1):
            self.copy(q, 2, 0, 0).start()
            self.copy(q, 2, 0, 1).start()
        p = self.p
        self.w[pl.ds(pl.multiple_of(p.mp * self.depth, self.depth), self.depth), :] = self.shard[...]

    def run(self):
        for q in (0, 1):
            self.wait(q, 1, 0, 0)
            self.copy(q, 1, 0, 2).start()
            self.wait(q, 1, 0, 1)
            self.copy(q, 1, 0, 3).start()
        for q in (0, 1):
            for o in (-1, 1):
                self.copy(q, 2, o, 0).start()
                self.copy(q, 2, o, 1).start()
        for q in (0, 1):
            self.wait(q, 2, 0, 0)
            self.copy(q, 2, 0, 2).start()
            self.wait(q, 2, 0, 1)
            self.copy(q, 2, 0, 3).start()
        for q in (0, 1):
            self.wait(q, 1, 0, 2)
            self.wait(q, 1, 0, 3)
            self.copy(q, 2, 2, 0).start()
            self.copy(q, 2, 2, 1).start()
        for o in (-1, 1, 2):
            for q in (0, 1):
                self.wait(q, 2, o, 0)
                self.copy(q, 2, o, 2).start()
                self.wait(q, 2, o, 1)
                self.copy(q, 2, o, 3).start()
        for o in (0, -1, 1, 2):
            for q in (0, 1):
                self.wait(q, 2, o, 2)
                self.wait(q, 2, o, 3)
        self.all_of(self.dsent, self.dgot).wait_recv()

    def drain(self):
        self.all_of(self.sent, self.dgot).wait_send()
        self.all_of(self.dsent, self.dgot).wait_send()


class Scatter:
    STEPS = (2, 1, -1, 0)

    def __init__(self, place, refs, sems):
        self.p = place
        self.gs, self.gd, self.g, self.l1, self.l2, self.l3, self.l4, self.turned, self.right = refs
        self.sent, self.drecv, self.recv, self.recv2 = sems
        self.half = self.g.shape[3] // 2

    def cols(self, q):
        return pl.ds(q * self.half, self.half)

    def order(self, q):
        p = self.p
        return [p.along(p.x if q == 0 else p.y, steps) for steps in self.STEPS]

    def block(self, q, first, second):
        return (first, second) if q == 0 else (second, first)

    def ring1(self, q, steps):
        p = self.p
        return p.along(p.y if q == 0 else p.x, steps)

    def group(self, q, k):
        at = self.ring1(q, self.STEPS[k])
        return (at, slice(None)) if q == 0 else (slice(None), at)

    def pair(self, q, first, low):
        if q == 0:
            return self.g.at[first, pl.ds(low, 2), :, self.cols(q)]
        return self.g.at[pl.ds(low, 2), first, :, self.cols(q)]

    def copy1(self, q, d):
        src = self.pair(q, self.ring1(q, 2), 2 * d)
        return remote(src, self.l1.at[q, d], self.sent.at[1], self.recv.at[0, q, d],
                      {"mp": self.p.chip(1 - q, 1 if d == 0 else -1)})

    def copy2(self, q, d, k):
        to = 1 if d == 0 else -1
        a, b = self.block(q, self.ring1(q, to), self.order(q)[k])
        return remote(self.g.at[a, b, :, self.cols(q)], self.l2.at[q, d, k],
                      self.sent.at[2], self.recv2.at[q, d, k], {"mp": self.p.chip(1 - q, to)})

    def copy3(self, q, d):
        a, b = self.block(q, self.ring1(q, 0), self.order(q)[0])
        n = self.g.shape[2] // 2
        return remote(self.g.at[a, b, pl.ds(d * n, n), self.cols(q)], self.l3.at[q, d],
                      self.sent.at[3], self.recv.at[1, q, d],
                      {"mp": self.p.chip(q, 1 if d == 0 else -1)})

    def copy4(self, q, d):
        a, b = self.block(q, self.ring1(q, 0), self.order(q)[1 + d])
        return remote(self.g.at[a, b, :, self.cols(q)], self.l4.at[q, d],
                      self.sent.at[4], self.recv.at[2, q, d],
                      {"mp": self.p.chip(q, 1 if d == 0 else -1)})

    def exchange(self, q, k):
        index = (*self.group(q, k), slice(None), self.cols(q))
        return remote(self.gs.at[index], self.gd.at[index], self.sent.at[0], self.drecv.at[q, k],
                      {"dp": 1 - self.p.core})

    def turn(self, left):
        per = self.g.shape[1] * self.g.shape[2]

        def one(n, _):
            block = left(pl.ds(pl.multiple_of(n * per, per), per)).T
            self.turned[n // SIDE, lax.rem(n, SIDE)] = block.reshape(SIDE, self.g.shape[2], block.shape[1])
            return 0

        lax.fori_loop(0, 2 * SIDE, one, 0)

    def product(self, core, q, k):
        rows = self.turned[(core, *self.group(q, k))]
        rows = rows.reshape(-1, rows.shape[2])
        value = jnp.dot(rows, self.right[:, self.cols(q)], preferred_element_type=F32)
        return value.reshape(SIDE, self.g.shape[2], self.half)

    def other(self, q, k):
        index = (*self.group(q, k), slice(None), self.cols(q))
        self.gs[index] = self.product(1 - self.p.core, q, k).astype(BF16)
        self.exchange(q, k).start()

    def own(self, q, k):
        index = (*self.group(q, k), slice(None), self.cols(q))
        value = self.product(self.p.core, q, k)
        self.exchange(q, k).wait_recv()
        self.g[index] = (value + self.gd[index].astype(F32)).astype(BF16)
        if k == 0:
            self.copy1(q, 0).start()
            self.copy1(q, 1).start()

    def products(self):
        parts = [(q, k) for k in range(SIDE) for q in (0, 1)]
        ahead = 3
        for n in range(len(parts) + ahead):
            if n < len(parts):
                self.other(*parts[n])
            if n >= ahead:
                self.own(*parts[n - ahead])

    def add(self, index, value):
        self.g[index] = (self.g[index].astype(F32) + value.astype(F32)).astype(BF16)

    def arrived(self, q, k):
        self.copy2(q, 0, k).wait_recv()
        self.copy2(q, 1, k).wait_recv()
        return self.l2[q, 0, k].astype(F32) + self.l2[q, 1, k].astype(F32)

    def run(self, finish):
        n = self.g.shape[2] // 2
        index = lambda q, k: (*self.block(q, self.ring1(q, 0), self.order(q)[k]), slice(None), self.cols(q))
        for d in (0, 1):
            for q in (0, 1):
                self.copy1(q, d).wait_recv()
                first = self.ring1(q, 1 if d == 0 else -1)
                for k in (0, 1):
                    a, b = self.block(q, first, 2 * d + k)
                    self.add((a, b, slice(None), self.cols(q)), self.l1[q, d, k])
                self.copy2(q, d, 0).start()
                self.copy2(q, d, 1).start()
        for q in (0, 1):
            self.add(index(q, 0), self.arrived(q, 0))
            self.copy3(q, 0).start()
            self.copy3(q, 1).start()
            for k in (2, 3):
                self.copy2(q, 0, k).start()
                self.copy2(q, 1, k).start()
        for d in (0, 1):
            for q in (0, 1):
                self.add(index(q, 1 + d), self.arrived(q, 1 + d))
                a, b, _, cols = index(q, 1 + d)
                self.copy3(q, d).wait_recv()
                self.add((a, b, pl.ds(d * n, n), cols), self.l3[q, d])
                self.copy4(q, d).start()
        for q in (0, 1):
            value = self.g[index(q, 3)].astype(F32) + self.arrived(q, 3)
            self.copy4(q, 0).wait_recv()
            self.copy4(q, 1).wait_recv()
            finish(q, value + self.l4[q, 0].astype(F32) + self.l4[q, 1].astype(F32))

    def drain(self):
        for n, ref in enumerate((self.gd, self.l1, self.l2, self.l3, self.l4)):
            remote(ref, ref, self.sent.at[n], self.drecv.at[0, 0], {"dp": 1 - self.p.core}).wait_send()


def step_kernel(sections, loss_scale, *refs):
    (
        h_inputs, h_tangents, h_targets, h_target_jac, mask, batch_order, h_encoder, h_shard, h_head,
        o_layer, o_head, o_loss,
        inputs, tangents, targets, target_jac, shard, head,
        w, wt, head_t, xin, xout, mix, cot, pin, pout, pre, thb, cin, cpin, cout, cpout, mixp, cotp,
        o_layer_buf, coef, wantp, count_out, count_in, loss_out, loss_in, loss_sum, loss_land, head_out, head_land,
        loads, stored, relayed, frecv, brecv,
        gsent, grecv1, grecv2, dsent, dgot,
        csend, crecv, lsend, lrecv, zsend, zrecv,
        *scatter,
    ) = refs
    layer_refs, layer_sems = scatter[:9], scatter[9:13]
    head_refs, head_sems = scatter[13:22], scatter[22:26]
    n_mb, rows, width = xin.shape
    rank = cin.shape[1]
    out_width = head.shape[1]
    tile = width // PIECES
    place = Place(sections)
    s, core, first, last = place.s, place.core, place.first, place.last
    chips = SIDE * SIDE

    encoder = head_t.at[pl.ds(0, h_encoder.shape[0])]

    def load(n):
        pairs = (
            (h_shard, shard), (h_inputs, inputs), (h_tangents, tangents), (h_encoder, encoder),
            (h_targets, targets), (h_target_jac, target_jac), (h_head, head),
        )
        return pltpu.make_async_copy(pairs[n][0], pairs[n][1], loads.at[n])

    for n in range(7):
        load(n).start()
    knock(place)

    @pl.when(first)
    def _():
        for n in (1, 2, 3):
            load(n).wait()
        primal = inputs[...].astype(F32)
        for m in range(n_mb):
            lhs = jnp.concatenate(
                [tangents[m], first_row(primal[m : m + 1], rows - rank).astype(BF16)], axis=0
            )
            lifted = jnp.dot(lhs, encoder[...], preferred_element_type=F32).astype(BF16)
            xin[m] = lifted
            pin[m] = lifted[rank:].astype(F32)[0:1]

    load(0).wait()
    enter()
    gather = Gather(place, shard, w, (gsent, grecv1, grecv2, dsent, dgot))
    gather.begin()
    gather.run()
    for n in (4, 5, 6):
        load(n).wait()

    @pl.when(jnp.logical_not(first))
    def _():
        for n in (1, 2, 3):
            load(n).wait()

    def count_copy(step):
        other = lax.rem(place.mp + step, chips)
        return remote(count_out, count_in.at[place.mp], csend.at[0], crecv.at[0], {"mp": other})

    def all_counts():
        ref = count_in.at[pl.ds(0, chips - 1)]
        return remote(ref, ref, csend.at[0], crecv.at[0], {"dp": 1 - core})

    def all_losses():
        ref = loss_in.at[pl.ds(0, 2 * chips - 1)]
        return remote(ref, ref, lsend.at[0], lrecv.at[0], {"dp": 1 - core})

    def turned_into(target, source):
        high, wide = source.shape
        step = 512 if high % 512 == 0 and wide % 512 == 0 else min(high, wide)
        count = wide // step

        def turn(n, _):
            a = pl.ds(pl.multiple_of((n // count) * step, step), step)
            b = pl.ds(pl.multiple_of(lax.rem(n, count) * step, step), step)
            target[b, a] = source[a, b].T
            return 0

        lax.fori_loop(0, (high // step) * count, turn, 0)

    @pl.when(last)
    def _():
        totals = 1.0 + jnp.sum(mask[...].astype(F32), axis=1, keepdims=True)
        where = lax.broadcasted_iota(jnp.int32, (n_mb, n_mb), 0) == jnp.broadcast_to(
            batch_order[...], (n_mb, n_mb)
        )
        where = where.astype(F32)
        count_out[...] = jnp.zeros_like(count_out)
        count_out[0:1, 0:n_mb] = jnp.sum(where * totals, axis=0, keepdims=True)
        count_in[place.mp] = count_out[...]
        lax.fori_loop(1, chips, lambda i, _: (count_copy(i).start(), 0)[1], 0)
        turned_into(head_t, head)
        all_counts().wait_recv()
        counts = jnp.sum(count_in[...], axis=0)[0:1, 0:n_mb]
        inverse = 1.0 / jnp.sum(where * counts, axis=1, keepdims=True)
        row = lax.broadcasted_iota(jnp.int32, (rows, 1), 0)
        ranks = totals.astype(jnp.int32) - 1
        primal_wanted = targets[...].astype(F32)
        for m in range(n_mb):
            present = jnp.logical_or(row < ranks[m : m + 1], row == rank)
            coef[m] = jnp.where(present, inverse[m : m + 1], 0.0)
            wantp[m] = primal_wanted[m : m + 1]
        loss_out[...] = jnp.zeros_like(loss_out)

    late = s >= sections // 2

    @pl.when(late)
    def _():
        turned_into(wt, w)

    def fcopy(m, j):
        cols = pl.ds(j * tile, tile)
        return remote(
            xout.at[m, pl.ds(0, rank), cols], xin.at[m, pl.ds(0, rank), cols],
            relayed.at[0], frecv.at[m, 0], {"section": place.nxt},
        )

    def fpcopy(m):
        return remote(
            pout.at[m], pin.at[m], relayed.at[1], frecv.at[m, 1], {"section": place.nxt}
        )

    def bcopy(m, j):
        cols = pl.ds(j * tile, tile)
        return remote(
            cout.at[m, :, cols], cin.at[m, :, cols],
            relayed.at[2], brecv.at[m, 0], {"section": place.prv},
        )

    def bpcopy(m):
        return remote(
            cpout.at[m], cpin.at[m], relayed.at[3], brecv.at[m, 1], {"section": place.prv}
        )

    def forward(m, span, sending):
        @pl.when(jnp.logical_not(first))
        def _():
            for i in range(span):
                ref = xin.at[m + i, pl.ds(0, rank)]
                remote(ref, ref, relayed.at[0], frecv.at[m + i, 0], {"section": place.nxt}).wait_recv()
                fpcopy(m + i).wait_recv()
                xin[m + i, pl.ds(rank, rows - rank), :] = first_row(pin[m + i], rows - rank).astype(BF16)

        for j in range(PIECES):
            cols = pl.ds(j * tile, tile)
            both = jnp.dot(
                xin[pl.ds(m, span)].reshape(span * rows, width), w[:, cols], preferred_element_type=F32
            )
            for i in range(span):
                acc = both[i * rows : i * rows + rows]
                th = jnp.tanh(acc[rank : rank + 1, :])
                slope = 1.0 - th * th
                tangent = acc[:rank, :]
                pre[m + i, :, cols] = tangent
                thb[m + i, :, cols] = th
                moved = xin[m + i, pl.ds(0, rank), cols].astype(F32) + slope * tangent
                xout[m + i, pl.ds(0, rank), cols] = moved.astype(BF16)
                primal = (pin[m + i, :, cols] + th).astype(BF16).astype(F32)
                pout[m + i, :, cols] = primal
                xout[m + i, pl.ds(rank, rows - rank), cols] = first_row(primal, rows - rank).astype(BF16)
                if sending:
                    fcopy(m + i, j).start()
        if sending:
            for i in range(span):
                fpcopy(m + i).start()

    def loss_copy(step):
        plane = 2 * chips
        me = core * chips + place.mp
        other = lax.rem(me + step, plane)
        return remote(
            loss_out, loss_in.at[me], lsend.at[0], lrecv.at[0],
            {"dp": other // chips, "mp": lax.rem(other, chips)},
        )

    def objective(m, span):
        step = min(256, out_width)
        total = jnp.zeros((1, 1), F32)
        for n in range(out_width // step):
            cols = pl.ds(n * step, step)
            outputs = jnp.dot(
                xout[pl.ds(m, span)].reshape(span * rows, width), head[:, cols],
                preferred_element_type=F32,
            )
            for i in range(span):
                wanted = jnp.concatenate(
                    [
                        target_jac[m + i, :, cols].astype(F32),
                        first_row(wantp[m + i, :, cols], rows - rank),
                    ],
                    axis=0,
                )
                mismatch = outputs[i * rows : (i + 1) * rows] - wanted
                weighted = coef[m + i] * mismatch
                total = total + jnp.sum(
                    jnp.sum(weighted * mismatch, axis=0, keepdims=True), axis=1, keepdims=True
                )
                rounded = (2.0 * weighted).astype(BF16)
                cot[m + i, :, cols] = rounded
                cotp[m + i, :, cols] = rounded[rank:].astype(F32)[0:1]
        loss_out[...] = loss_out[...] + jnp.broadcast_to(total, loss_out.shape)
        for j in range(PIECES):
            cols = pl.ds(j * tile, tile)
            grads = jnp.dot(
                cot[pl.ds(m, span)].reshape(span * rows, out_width), head_t[:, cols],
                preferred_element_type=F32,
            ).astype(BF16)
            for i in range(span):
                cin[m + i, :, cols] = grads[i * rows : i * rows + rank, :]
                cpin[m + i, :, cols] = grads[i * rows + rank : (i + 1) * rows, :].astype(F32)[0:1]

    def mixed(m):
        for j in range(PIECES):
            cols = pl.ds(j * tile, tile)
            upstream = cin[m, :, cols].astype(F32)
            th = thb[m, :, cols]
            slope = 1.0 - th * th
            mix[m, pl.ds(0, rank), cols] = (upstream * slope).astype(BF16)
            total = jnp.sum(upstream * pre[m, :, cols], axis=0, keepdims=True)
            primal = cpin[m, :, cols] * slope - 2.0 * total * th * slope
            mixp[m, :, cols] = primal
            mix[m, pl.ds(rank, rows - rank), cols] = first_row(primal, rows - rank).astype(BF16)

    def backward(m, span):
        for i in range(span):
            mixed(m + i)

        @pl.when(jnp.logical_not(first))
        def _():
            for j in range(PIECES):
                cols = pl.ds(j * tile, tile)
                both = jnp.dot(
                    mix[pl.ds(m, span)].reshape(span * rows, width), wt[:, cols],
                    preferred_element_type=F32,
                )
                for i in range(span):
                    back = both[i * rows : (i + 1) * rows]
                    cout[m + i, :, cols] = (cin[m + i, :, cols].astype(F32) + back[:rank]).astype(BF16)
                    cpout[m + i, :, cols] = (
                        (cpin[m + i, :, cols] + back[rank : rank + 1]).astype(BF16).astype(F32)
                    )
                bcopy(m, j).start()
            bpcopy(m).start()
            for i in range(1, span):
                for j in range(PIECES):
                    bcopy(m + i, j).start()
                bpcopy(m + i).start()

    heads = Scatter(place, head_refs, head_sems)
    sums = Scatter(place, layer_refs, layer_sems)

    def compact(tangent, primal):
        def take(cols):
            block = tangent[:, pl.ds(0, rank), cols]
            rest = stacked_rows(lambda m: primal[m, :, cols], n_mb, 16, block.shape[2])
            return jnp.concatenate(
                [block.reshape(n_mb * rank, block.shape[2]), rest.astype(BF16)], axis=0
            )

        return take

    @pl.when(last)
    def _():
        span = 2

        def group(g, _):
            forward(g * span, span, False)
            objective(g * span, span)
            backward(g * span, span)
            return 0

        lax.fori_loop(0, n_mb // span, group, 0)
        loss_in[core * chips + place.mp] = loss_out[...]
        lax.fori_loop(1, 2 * chips, lambda i, _: (loss_copy(i).start(), 0)[1], 0)
        sums.turn(compact(xin, pin))

    @pl.when(jnp.logical_not(last))
    def _():
        lax.fori_loop(0, n_mb, lambda m, _: (forward(m, 1, True), 0)[1], 0)

        @pl.when(jnp.logical_not(jnp.logical_or(late, first)))
        def _():
            turned_into(wt, w)

        sums.turn(compact(xin, pin))

        def back(m, _):
            ref = cin.at[m]
            remote(ref, ref, relayed.at[2], brecv.at[m, 0], {"section": place.prv}).wait_recv()
            bpcopy(m).wait_recv()
            backward(m, 1)
            return 0

        lax.fori_loop(0, n_mb, back, 0)

    def section_copy(step, what):
        other = lax.rem(place.s + step, sections)
        if what == 0:
            return remote(head_out.at[other], head_land, zsend.at[0], zrecv.at[0], {"section": other})
        return remote(loss_sum, loss_land, zsend.at[1], zrecv.at[1], {"section": other})

    @pl.when(last)
    def _():
        heads.turn(compact(xout, pout))
        heads.right[...] = compact(cot, cotp)(slice(None))
        heads.products()

        def finish(q, value):
            per = out_width // sections
            for k in range(heads.half // per):
                head_out[q * (heads.half // per) + k] = value[:, k * per : (k + 1) * per]

        heads.run(finish)
        all_losses().wait_recv()
        loss_sum[...] = jnp.sum(loss_in[...], axis=0) * loss_scale

        def spread(i, _):
            section_copy(i, 0).start()
            section_copy(i, 1).start()
            return 0

        lax.fori_loop(1, sections, spread, 0)
        o_head[...] = head_out[sections - 1]
        o_loss[...] = loss_sum[0:1, 0:1]

    sums.right[...] = compact(mix, mixp)(slice(None))
    sums.products()

    def layer_out(q):
        cols = pl.ds(q * sums.half, sums.half)
        return pltpu.make_async_copy(o_layer_buf.at[:, cols], o_layer.at[:, cols], stored.at[q])

    def finish_layer(q, value):
        o_layer_buf[:, pl.ds(q * sums.half, sums.half)] = value
        layer_out(q).start()

    sums.run(finish_layer)

    @pl.when(jnp.logical_not(last))
    def _():
        section_copy(1, 0).wait_recv()
        section_copy(1, 1).wait_recv()
        o_head[...] = head_land[...]
        o_loss[...] = loss_land[0:1, 0:1]

    def relays_left(ref, n):
        remote(ref, ref, relayed.at[n], frecv.at[0, 0], {"section": place.nxt}).wait_send()

    @pl.when(jnp.logical_not(last))
    def _():
        relays_left(cin, 0)
        relays_left(pout, 1)

    @pl.when(jnp.logical_not(first))
    def _():
        relays_left(cout, 2)
        relays_left(cpout, 3)

    gather.drain()
    sums.drain()
    layer_out(0).wait()
    layer_out(1).wait()

    @pl.when(last)
    def _():
        heads.drain()
        all_counts().wait_send()
        all_losses().wait_send()
        for ref, n in ((head_out, 0), (loss_in, 1)):
            ref = ref.at[pl.ds(0, sections - 1)]
            remote(ref, ref, zsend.at[n], zrecv.at[n], {"section": place.nxt}).wait_send()


def scatter_scratch(rows, cols, depth):
    half = cols // 2
    dma = pltpu.SemaphoreType.DMA
    part = (SIDE, SIDE, rows, cols)
    return [
        pltpu.VMEM(part, BF16),
        pltpu.VMEM(part, BF16),
        pltpu.VMEM(part, BF16),
        pltpu.VMEM((2, 2, 2, rows, half), BF16),
        pltpu.VMEM((2, 2, SIDE, rows, half), BF16),
        pltpu.VMEM((2, 2, rows // 2, half), BF16),
        pltpu.VMEM((2, 2, rows, half), BF16),
        pltpu.VMEM((2, SIDE, SIDE, rows, depth), BF16),
        pltpu.VMEM((depth, cols), BF16),
        dma((5,)), dma((2, SIDE)), dma((3, 2, 2)), dma((2, 2, SIDE)),
    ]


def local(
    inputs, tangents, targets, target_jac, rank_mask, batch_order, encoder, layers, head_weight
):
    n_mb, rank, _ = tangents.shape
    width = layers.shape[2]
    out_width = head_weight.shape[1]
    sections = lax.axis_size("section")
    chips = SIDE * SIDE
    own = width // (2 * chips)
    per = out_width // sections
    dma = pltpu.SemaphoreType.DMA
    vmem = pl.BlockSpec(memory_space=pltpu.VMEM)
    hbm = pl.BlockSpec(memory_space=pl.ANY)
    like = lambda a: pltpu.VMEM(a.shape, a.dtype)
    row = pltpu.VMEM((n_mb, 1, width), F32)
    block = pltpu.VMEM((n_mb, ROWS, width), BF16)
    send = pltpu.VMEM((n_mb, rank, width), BF16)
    grad_layer, grad_head, loss = pl.pallas_call(
        functools.partial(step_kernel, sections, 1.0 / (lax.axis_size("dp") * n_mb * out_width)),
        out_shape=(
            jax.ShapeDtypeStruct((own, width), F32),
            jax.ShapeDtypeStruct((own, per), F32),
            jax.ShapeDtypeStruct((1, 1), F32),
        ),
        in_specs=[hbm] * 4 + [vmem] * 2 + [hbm] * 3,
        out_specs=(hbm, vmem, vmem),
        scratch_shapes=[
            like(inputs), like(tangents), like(targets), like(target_jac),
            like(layers[0]), like(head_weight),
            pltpu.VMEM((width, width), BF16),
            pltpu.VMEM((width, width), BF16),
            pltpu.VMEM((out_width, width), BF16),
            block, block, block,
            pltpu.VMEM((n_mb, ROWS, out_width), BF16),
            row, row,
            pltpu.VMEM((n_mb, rank, width), F32),
            row, send, row, send, row, row,
            pltpu.VMEM((n_mb, 1, out_width), F32),
            pltpu.VMEM((own, width), F32),
            pltpu.VMEM((n_mb, ROWS, 1), F32),
            pltpu.VMEM((n_mb, 1, out_width), F32),
            pltpu.VMEM((8, 128), F32),
            pltpu.VMEM((chips, 8, 128), F32),
            pltpu.VMEM((8, 128), F32),
            pltpu.VMEM((2 * chips, 8, 128), F32),
            pltpu.VMEM((8, 128), F32),
            pltpu.VMEM((8, 128), F32),
            pltpu.VMEM((sections, own, per), F32),
            pltpu.VMEM((own, per), F32),
            dma((7,)), dma((2,)), dma((4,)), dma((n_mb, 2)), dma((n_mb, 2)),
            dma, dma((2, 4)), dma((2, SIDE, 4)), dma, dma,
            dma((1,)), dma((1,)), dma((1,)), dma((1,)), dma((2,)), dma((2,)),
            *scatter_scratch(own, width, n_mb * rank + 16),
            *scatter_scratch(own, out_width, n_mb * rank + 16),
        ],
        compiler_params=pltpu.CompilerParams(
            collective_id=0, has_side_effects=True, vmem_limit_bytes=67043328
        ),
        name="step",
    )(
        inputs, tangents, targets, target_jac, rank_mask, batch_order, encoder, layers[0],
        head_weight,
    )
    return grad_layer[None], grad_head, loss.reshape(())


def solution(mesh):
    in_specs = (
        P(("dp", "mp"), None),
        P(("dp", "mp"), None, None),
        P(("dp", "mp"), None),
        P(("dp", "mp"), None, None),
        P(("dp", "mp"), None),
        P(("dp", "mp"), None),
        P(),
        P("section", "mp", None),
        P(),
    )
    out_specs = (P("section", ("dp", "mp"), None), P(("dp", "mp"), "section"), P())
    return jax.shard_map(local, mesh=mesh, in_specs=in_specs, out_specs=out_specs, check_vma=False)
```

```python
import functools

import jax
import jax.numpy as jnp
from jax import lax
from jax.experimental import pallas as pl
from jax.experimental.pallas import tpu as pltpu
from jax.sharding import PartitionSpec as P

SIDE = 4
ROWS = 48
PIECES = 2
MESH = pl.DeviceIdType.MESH
BF16, F32 = jnp.bfloat16, jnp.float32


def first_row(row, height):
    rows = lax.broadcasted_iota(jnp.int32, (height, row.shape[1]), 0)
    return jnp.where(rows == 0, jnp.broadcast_to(row, (height, row.shape[1])), 0.0)


def stacked_rows(get_row, count, height, width):
    rows = lax.broadcasted_iota(jnp.int32, (height, width), 0)
    block = jnp.zeros((height, width), F32)
    for m in range(count):
        block = jnp.where(rows == m, jnp.broadcast_to(get_row(m), (height, width)), block)
    return block


class Place:
    def __init__(self, sections):
        self.sections = sections
        self.core = lax.axis_index("dp")
        self.s = lax.axis_index("section")
        self.mp = lax.axis_index("mp")
        self.y = self.mp // SIDE
        self.x = lax.rem(self.mp, SIDE)
        self.first = self.s == 0
        self.last = self.s == sections - 1
        self.middle = jnp.logical_not(jnp.logical_or(self.first, self.last))
        self.carrier = jnp.logical_and(self.middle, self.core == 1)
        self.nxt = lax.rem(self.s + 1, sections)
        self.prv = lax.rem(self.s + sections - 1, sections)

    def along(self, coordinate, steps):
        return lax.rem(coordinate + steps + SIDE, SIDE)

    def chip(self, axis, steps):
        if axis == 0:
            return self.y * SIDE + self.along(self.x, steps)
        return self.along(self.y, steps) * SIDE + self.x


def remote(src, dst, send, recv, device_id):
    return pltpu.make_async_remote_copy(
        src_ref=src, dst_ref=dst, send_sem=send, recv_sem=recv,
        device_id=device_id, device_id_type=MESH,
    )


def neighbours(place):
    for axis in (0, 1):
        for steps in (1, -1):
            yield {"mp": place.chip(axis, steps)}
    yield {"dp": 1 - place.core}
    for section in (place.nxt, place.prv):
        for core in (0, 1):
            yield {"dp": core, "section": section}


def knock(place):
    barrier = pltpu.get_barrier_semaphore()
    for device in neighbours(place):
        pl.semaphore_signal(barrier, inc=1, device_id=device, device_id_type=MESH)


def enter():
    pl.semaphore_wait(pltpu.get_barrier_semaphore(), 9)


class Gather:
    def __init__(self, place, shard, w, sems):
        self.p, self.shard, self.w = place, shard, w
        self.sent, self.recv1, self.recv2, self.dsent, self.dgot = sems
        self.depth = shard.shape[0]
        self.piece = self.depth // 4

    def rows(self, q, core, step1, step2, half):
        p = self.p
        dx, dy = (step1, step2) if q == 0 else (step2, step1)
        chip = p.along(p.y, dy) * SIDE + p.along(p.x, dx)
        start = chip * self.depth + core * (2 * self.piece) + q * self.piece
        length = self.piece
        if half is not None:
            length = self.piece // 2
            start = start + half * length
        return pl.ds(pl.multiple_of(start, length), length)

    def copy(self, q, phase, o, e):
        p = self.p
        axis = q if phase == 1 else 1 - q
        to = 1 if e in (0, 2) else -1
        back = {0: 0, 1: 0, 2: -1, 3: 1}[e]
        half = {0: None, 1: None, 2: 0, 3: 1}[e]
        step1, step2 = (back, 0) if phase == 1 else (o, back)
        dst = self.w.at[self.rows(q, p.core, step1, step2, half)]
        src = dst
        if step1 == 0 and step2 == 0:
            src = self.shard.at[pl.ds(pl.multiple_of(p.core * (2 * self.piece) + q * self.piece, self.piece), self.piece)]
        return remote(src, dst, self.sent, self.recv(phase, q, o, e), {"mp": p.chip(axis, to)})

    def recv(self, phase, q, o, e):
        return self.recv1.at[q, e] if phase == 1 else self.recv2.at[q, o % SIDE, e]

    def arrived(self, q, phase, o, e):
        p = self.p
        away = {0: -1, 1: 1, 2: -2, 3: 2}[e]
        half = {0: None, 1: None, 2: 0, 3: 1}[e]
        step1, step2 = (away, 0) if phase == 1 else (o, away)
        return self.p, q, step1, step2, half

    def wait(self, q, phase, o, e):
        p, q, step1, step2, half = self.arrived(q, phase, o, e)
        dst = self.w.at[self.rows(q, p.core, step1, step2, half)]
        remote(dst, dst, self.sent, self.recv(phase, q, o, e), {"mp": p.chip(0, 1)}).wait_recv()
        remote(dst, dst, self.dsent, self.dgot, {"dp": 1 - p.core}).start()

    def all_of(self, send, recv):
        ref = self.w.at[pl.ds(0, (SIDE * SIDE - 1) * 2 * self.piece)]
        return remote(ref, ref, send, recv, {"dp": 1 - self.p.core})

    def begin(self):
        for q in (0, 1):
            self.copy(q, 1, 0, 0).start()
            self.copy(q, 1, 0, 1).start()
        for q in (0, 1):
            self.copy(q, 2, 0, 0).start()
            self.copy(q, 2, 0, 1).start()
        p = self.p
        self.w[pl.ds(pl.multiple_of(p.mp * self.depth, self.depth), self.depth), :] = self.shard[...]

    def run(self):
        for q in (0, 1):
            self.wait(q, 1, 0, 0)
            self.copy(q, 1, 0, 2).start()
            self.wait(q, 1, 0, 1)
            self.copy(q, 1, 0, 3).start()
        for q in (0, 1):
            for o in (-1, 1):
                self.copy(q, 2, o, 0).start()
                self.copy(q, 2, o, 1).start()
        for q in (0, 1):
            self.wait(q, 2, 0, 0)
            self.copy(q, 2, 0, 2).start()
            self.wait(q, 2, 0, 1)
            self.copy(q, 2, 0, 3).start()
        for q in (0, 1):
            self.wait(q, 1, 0, 2)
            self.wait(q, 1, 0, 3)
            self.copy(q, 2, 2, 0).start()
            self.copy(q, 2, 2, 1).start()
        for o in (-1, 1, 2):
            for q in (0, 1):
                self.wait(q, 2, o, 0)
                self.copy(q, 2, o, 2).start()
                self.wait(q, 2, o, 1)
                self.copy(q, 2, o, 3).start()
        for o in (0, -1, 1, 2):
            for q in (0, 1):
                self.wait(q, 2, o, 2)
                self.wait(q, 2, o, 3)
        self.all_of(self.dsent, self.dgot).wait_recv()

    def drain(self):
        self.all_of(self.sent, self.dgot).wait_send()
        self.all_of(self.dsent, self.dgot).wait_send()


class Scatter:
    STEPS = (2, 1, -1, 0)

    def __init__(self, place, refs, sems):
        self.p = place
        self.gs, self.gd, self.g, self.l1, self.l2, self.l3, self.l4, self.turned, self.right = refs
        self.sent, self.drecv, self.recv, self.recv2, self.recv4 = sems
        self.half = self.g.shape[3] // 2

    def cols(self, q):
        return pl.ds(q * self.half, self.half)

    def order(self, q):
        p = self.p
        return [p.along(p.x if q == 0 else p.y, steps) for steps in self.STEPS]

    def block(self, q, first, second):
        return (first, second) if q == 0 else (second, first)

    def ring1(self, q, steps):
        p = self.p
        return p.along(p.y if q == 0 else p.x, steps)

    def group(self, q, k):
        at = self.ring1(q, self.STEPS[k])
        return (at, slice(None)) if q == 0 else (slice(None), at)

    def pair(self, q, first, low):
        if q == 0:
            return self.g.at[first, pl.ds(low, 2), :, self.cols(q)]
        return self.g.at[pl.ds(low, 2), first, :, self.cols(q)]

    def copy1(self, q, d):
        src = self.pair(q, self.ring1(q, 2), 2 * d)
        return remote(src, self.l1.at[q, d], self.sent.at[1], self.recv.at[0, q, d],
                      {"mp": self.p.chip(1 - q, 1 if d == 0 else -1)})

    def copy2(self, q, d, b):
        to = 1 if d == 0 else -1
        at = self.block(q, self.ring1(q, to), b)
        return remote(self.g.at[(*at, slice(None), self.cols(q))], self.l2.at[q, d, b],
                      self.sent.at[2], self.recv2.at[q, d, b], {"mp": self.p.chip(1 - q, to)})

    def copy3(self, q, d):
        a, b = self.block(q, self.ring1(q, 0), self.order(q)[0])
        n = self.g.shape[2] // 2
        return remote(self.g.at[a, b, pl.ds(d * n, n), self.cols(q)], self.l3.at[q, d],
                      self.sent.at[3], self.recv.at[1, q, d],
                      {"mp": self.p.chip(q, 1 if d == 0 else -1)})

    def copy4(self, q, d, h):
        a, b = self.block(q, self.ring1(q, 0), self.order(q)[1 + d])
        n = self.g.shape[2] // 2
        rows = pl.ds(h * n, n)
        return remote(self.g.at[a, b, rows, self.cols(q)], self.l4.at[q, d, rows],
                      self.sent.at[4], self.recv4.at[q, d, h],
                      {"mp": self.p.chip(q, 1 if d == 0 else -1)})

    def exchange(self, q, k):
        index = (*self.group(q, k), slice(None), self.cols(q))
        return remote(self.gs.at[index], self.gd.at[index], self.sent.at[0], self.drecv.at[q, k],
                      {"dp": 1 - self.p.core})

    def turn(self, left):
        per = self.g.shape[1] * self.g.shape[2]

        def one(n, _):
            block = left(pl.ds(pl.multiple_of(n * per, per), per)).T
            self.turned[n // SIDE, lax.rem(n, SIDE)] = block.reshape(SIDE, self.g.shape[2], block.shape[1])
            return 0

        lax.fori_loop(0, 2 * SIDE, one, 0)

    def product(self, core, q, k):
        rows = self.turned[(core, *self.group(q, k))]
        rows = rows.reshape(-1, rows.shape[2])
        value = jnp.dot(rows, self.right[:, self.cols(q)], preferred_element_type=F32)
        return value.reshape(SIDE, self.g.shape[2], self.half)

    def other(self, q, k):
        index = (*self.group(q, k), slice(None), self.cols(q))
        self.gs[index] = self.product(1 - self.p.core, q, k).astype(BF16)
        self.exchange(q, k).start()

    def own(self, q, k):
        index = (*self.group(q, k), slice(None), self.cols(q))
        value = self.product(self.p.core, q, k)
        self.exchange(q, k).wait_recv()
        self.g[index] = (value + self.gd[index].astype(F32)).astype(BF16)
        if k == 0:
            self.copy1(q, 0).start()
            self.copy1(q, 1).start()
        elif k < 3:
            d = k - 1
            self.copy2(q, d, 2 - 2 * d).start()
            self.copy2(q, d, 3 - 2 * d).start()

    def products(self):
        parts = [(q, k) for k in range(SIDE) for q in (0, 1)]
        ahead = 3
        for n in range(len(parts) + ahead):
            if n < len(parts):
                self.other(*parts[n])
            if n >= ahead:
                self.own(*parts[n - ahead])

    def add(self, index, value):
        self.g[index] = (self.g[index].astype(F32) + value.astype(F32)).astype(BF16)

    def arrived(self, q, k):
        b = self.order(q)[k]
        self.copy2(q, 0, b).wait_recv()
        self.copy2(q, 1, b).wait_recv()
        return self.l2[q, 0, b].astype(F32) + self.l2[q, 1, b].astype(F32)

    def run(self, finish):
        n = self.g.shape[2] // 2
        index = lambda q, k: (*self.block(q, self.ring1(q, 0), self.order(q)[k]), slice(None), self.cols(q))
        for d in (0, 1):
            for q in (0, 1):
                self.copy1(q, d).wait_recv()
                first = self.ring1(q, 1 if d == 0 else -1)
                for k in (0, 1):
                    a, b = self.block(q, first, 2 * d + k)
                    self.add((a, b, slice(None), self.cols(q)), self.l1[q, d, k])
                far = self.order(q)[0]
                low = jnp.where(far // 2 == d, far, 2 * d)
                self.copy2(q, d, low).start()
                self.copy2(q, d, 4 * d + 1 - low).start()
        for q in (0, 1):
            self.add(index(q, 0), self.arrived(q, 0))
            self.copy3(q, 0).start()
            self.copy3(q, 1).start()
        for d in (0, 1):
            for q in (0, 1):
                self.add(index(q, 1 + d), self.arrived(q, 1 + d))
                self.copy4(q, d, 1 - d).start()
        for d in (0, 1):
            for q in (0, 1):
                a, b, _, cols = index(q, 1 + d)
                self.copy3(q, d).wait_recv()
                self.add((a, b, pl.ds(d * n, n), cols), self.l3[q, d])
                self.copy4(q, d, d).start()
        for q in (0, 1):
            value = self.g[index(q, 3)].astype(F32) + self.arrived(q, 3)
            for d in (0, 1):
                self.copy4(q, d, 0).wait_recv()
                self.copy4(q, d, 1).wait_recv()
            finish(q, value + self.l4[q, 0].astype(F32) + self.l4[q, 1].astype(F32))

    def drain(self):
        for n, ref in enumerate((self.gd, self.l1, self.l2, self.l3, self.l4)):
            remote(ref, ref, self.sent.at[n], self.drecv.at[0, 0], {"dp": 1 - self.p.core}).wait_send()


def step_kernel(sections, loss_scale, *refs):
    (
        h_inputs, h_tangents, h_targets, h_target_jac, mask, batch_order, h_encoder, h_shard, h_head,
        o_layer, o_head, o_loss,
        inputs, tangents, targets, target_jac, shard, head,
        w, wt, head_t, xin, xout, mix, cot, pin, pout, pre, thb, cin, cpin, cout, cpout, mixp, cotp,
        o_layer_buf, coef, wantp, count_out, count_in, loss_out, loss_in, loss_sum, loss_land, head_out, head_land,
        loads, stored, relayed, frecv, brecv,
        gsent, grecv1, grecv2, dsent, dgot,
        csend, crecv, lsend, lrecv, zsend, zrecv, hsend, hrecv,
        *scatter,
    ) = refs
    layer_refs, layer_sems = scatter[:9], scatter[9:14]
    n_mb, rows, width = xout.shape
    rank = cin.shape[1]
    out_width = head.shape[1]
    part = pl.ds(0, out_width)
    head_refs = (
        layer_refs[0].at[:, :, :, part], scatter[14], layer_refs[2].at[:, :, :, part], *scatter[15:21]
    )
    head_sems = scatter[21:26]
    tile = width // PIECES
    place = Place(sections)
    s, core, first, last = place.s, place.core, place.first, place.last
    chips = SIDE * SIDE

    encoder = head_t.at[pl.ds(0, h_encoder.shape[0])]

    def load(n):
        pairs = (
            (h_shard, shard), (h_inputs, inputs), (h_tangents, tangents), (h_encoder, encoder),
            (h_targets, targets), (h_target_jac, target_jac), (h_head, head),
        )
        return pltpu.make_async_copy(pairs[n][0], pairs[n][1], loads.at[n])

    for n in range(7):
        load(n).start()
    knock(place)

    load(0).wait()
    enter()
    gather = Gather(place, shard, w, (gsent, grecv1, grecv2, dsent, dgot))
    gather.begin()

    @pl.when(first)
    def _():
        for n in (1, 2, 3):
            load(n).wait()
        primal = inputs[...].astype(F32)
        for m in range(n_mb):
            lhs = jnp.concatenate(
                [tangents[m], first_row(primal[m : m + 1], rows - rank).astype(BF16)], axis=0
            )
            lifted = jnp.dot(lhs, encoder[...], preferred_element_type=F32).astype(BF16)
            xin[m] = lifted
            pin[m] = lifted[rank:].astype(F32)[0:1]

    gather.run()
    for n in (4, 5, 6):
        load(n).wait()

    @pl.when(jnp.logical_not(first))
    def _():
        for n in (1, 2, 3):
            load(n).wait()

    def count_copy(step):
        other = lax.rem(place.mp + step, chips)
        return remote(count_out, count_in.at[place.mp], csend.at[0], crecv.at[0], {"mp": other})

    def all_counts():
        ref = count_in.at[pl.ds(0, chips - 1)]
        return remote(ref, ref, csend.at[0], crecv.at[0], {"dp": 1 - core})

    def all_losses():
        ref = loss_in.at[pl.ds(0, 2 * chips - 1)]
        return remote(ref, ref, lsend.at[0], lrecv.at[0], {"dp": 1 - core})

    def turned_into(target, source):
        high, wide = source.shape
        step = 512 if high % 512 == 0 and wide % 512 == 0 else min(high, wide)
        count = wide // step

        def turn(n, _):
            a = pl.ds(pl.multiple_of((n // count) * step, step), step)
            b = pl.ds(pl.multiple_of(lax.rem(n, count) * step, step), step)
            target[b, a] = source[a, b].T
            return 0

        lax.fori_loop(0, (high // step) * count, turn, 0)

    @pl.when(last)
    def _():
        totals = 1.0 + jnp.sum(mask[...].astype(F32), axis=1, keepdims=True)
        where = lax.broadcasted_iota(jnp.int32, (n_mb, n_mb), 0) == jnp.broadcast_to(
            batch_order[...], (n_mb, n_mb)
        )
        where = where.astype(F32)
        count_out[...] = jnp.zeros_like(count_out)
        count_out[0:1, 0:n_mb] = jnp.sum(where * totals, axis=0, keepdims=True)
        count_in[place.mp] = count_out[...]
        lax.fori_loop(1, chips, lambda i, _: (count_copy(i).start(), 0)[1], 0)
        turned_into(head_t, head)
        all_counts().wait_recv()
        counts = jnp.sum(count_in[...], axis=0)[0:1, 0:n_mb]
        inverse = 1.0 / jnp.sum(where * counts, axis=1, keepdims=True)
        row = lax.broadcasted_iota(jnp.int32, (rows, 1), 0)
        ranks = totals.astype(jnp.int32) - 1
        primal_wanted = targets[...].astype(F32)
        for m in range(n_mb):
            present = jnp.logical_or(row < ranks[m : m + 1], row == rank)
            coef[m] = jnp.where(present, inverse[m : m + 1], 0.0)
            wantp[m] = primal_wanted[m : m + 1]
        loss_out[...] = jnp.zeros_like(loss_out)

    late = s >= sections // 2

    @pl.when(jnp.logical_and(late, jnp.logical_or(last, place.carrier)))
    def _():
        turned_into(wt, w)

    def onward(slot, end):
        m = lax.rem(slot, n_mb)
        away = jnp.logical_or(slot >= n_mb, jnp.logical_and(jnp.logical_not(place.middle), core == 0))
        to_own = jnp.logical_and(away, end)
        taker = jnp.where(to_own, 0, 1)
        return taker, m + jnp.where(jnp.logical_and(away, jnp.logical_not(end)), n_mb, 0)

    def relayed_copy(slot, j, forth):
        to = place.nxt if forth else place.prv
        taker, there = onward(slot, to == (sections - 1 if forth else 0))
        device = {"dp": taker, "section": to}
        recv = frecv if forth else brecv
        kind = 0 if forth else 2
        if j == PIECES:
            landing = pin if forth else cpin
            return remote(cpout.at[slot], landing.at[there], relayed.at[kind + 1], recv.at[there, 1], device)
        cols = pl.ds(j * tile, tile)
        landing = xin.at[there, pl.ds(0, rank), cols] if forth else cin.at[there, :, cols]
        return remote(cout.at[slot, :, cols], landing, relayed.at[kind], recv.at[there, 0], device)

    def await_relayed(slot, forth):
        recv = frecv if forth else brecv
        ref = xin.at[slot, pl.ds(0, rank)] if forth else cin.at[slot]
        remote(ref, ref, relayed.at[0], recv.at[slot, 0], {"section": place.nxt}).wait_recv()
        ref = pin.at[slot] if forth else cpin.at[slot]
        remote(ref, ref, relayed.at[1], recv.at[slot, 1], {"section": place.nxt}).wait_recv()

    def relays_left(forth):
        kind = 0 if forth else 2
        for count, when in ((n_mb, jnp.logical_not(place.middle)), (2 * n_mb, place.carrier)):

            @pl.when(when)
            def _(count=count):
                for n, ref in ((kind, cin), (kind + 1, cpin)):
                    ref = ref.at[pl.ds(0, count)]
                    remote(ref, ref, relayed.at[n], frecv.at[0, 0], {"section": place.nxt}).wait_send()

    def hand_over(kind, slot):
        to = slot - n_mb
        pairs = ((xin, pin), (mix, mixp))[kind]
        for n, ref in enumerate(pairs):
            sem = 2 * kind + n
            remote(ref.at[slot], ref.at[to], hsend.at[sem], hrecv.at[sem], {"dp": 1 - core}).start()

    def handed(kind):
        pairs = ((xin, pin), (mix, mixp))[kind]
        for n, ref in enumerate(pairs):
            ref = ref.at[pl.ds(0, n_mb)]
            sem = 2 * kind + n
            yield remote(ref, ref, hsend.at[sem], hrecv.at[sem], {"dp": 1 - core})

    def blocks(ref, slots):
        return jnp.concatenate([ref[slot] for slot in slots], axis=0)

    def forward(slots, arriving, sending):
        if arriving:
            for slot in slots:
                await_relayed(slot, True)
                xin[slot, pl.ds(rank, rows - rank), :] = first_row(pin[slot], rows - rank).astype(BF16)
        for j in range(PIECES):
            cols = pl.ds(j * tile, tile)
            both = jnp.dot(blocks(xin, slots), w[:, cols], preferred_element_type=F32)
            for i, slot in enumerate(slots):
                acc = both[i * rows : i * rows + rows]
                th = jnp.tanh(acc[rank : rank + 1, :])
                slope = 1.0 - th * th
                tangent = acc[:rank, :]
                pre[slot, :, cols] = tangent.astype(BF16)
                thb[slot, :, cols] = th
                moved = xin[slot, pl.ds(0, rank), cols].astype(F32) + slope * tangent
                primal = (pin[slot, :, cols] + th).astype(BF16).astype(F32)
                if sending:
                    cout[slot, :, cols] = moved.astype(BF16)
                    cpout[slot, :, cols] = primal
                    relayed_copy(slot, j, True).start()
                else:
                    pout[slot, :, cols] = primal
                    xout[slot, pl.ds(0, rank), cols] = moved.astype(BF16)
                    xout[slot, pl.ds(rank, rows - rank), cols] = first_row(primal, rows - rank).astype(BF16)
        if sending:
            for slot in slots:
                relayed_copy(slot, PIECES, True).start()

    def loss_copy(step):
        plane = 2 * chips
        me = core * chips + place.mp
        other = lax.rem(me + step, plane)
        return remote(
            loss_out, loss_in.at[me], lsend.at[0], lrecv.at[0],
            {"dp": other // chips, "mp": lax.rem(other, chips)},
        )

    def objective(m, span):
        step = min(256, out_width)
        total = jnp.zeros((1, 1), F32)
        for n in range(out_width // step):
            cols = pl.ds(n * step, step)
            outputs = jnp.dot(
                xout[pl.ds(m, span)].reshape(span * rows, width), head[:, cols],
                preferred_element_type=F32,
            )
            for i in range(span):
                wanted = jnp.concatenate(
                    [
                        target_jac[m + i, :, cols].astype(F32),
                        first_row(wantp[m + i, :, cols], rows - rank),
                    ],
                    axis=0,
                )
                mismatch = outputs[i * rows : (i + 1) * rows] - wanted
                weighted = coef[m + i] * mismatch
                total = total + jnp.sum(
                    jnp.sum(weighted * mismatch, axis=0, keepdims=True), axis=1, keepdims=True
                )
                rounded = (2.0 * weighted).astype(BF16)
                cot[m + i, :, cols] = rounded
                cotp[m + i, :, cols] = rounded[rank:].astype(F32)[0:1]
        loss_out[...] = loss_out[...] + jnp.broadcast_to(total, loss_out.shape)
        for j in range(PIECES):
            cols = pl.ds(j * tile, tile)
            grads = jnp.dot(
                cot[pl.ds(m, span)].reshape(span * rows, out_width), head_t[:, cols],
                preferred_element_type=F32,
            ).astype(BF16)
            for i in range(span):
                cin[m + i, :, cols] = grads[i * rows : i * rows + rank, :]
                cpin[m + i, :, cols] = grads[i * rows + rank : (i + 1) * rows, :].astype(F32)[0:1]

    def mixed(m):
        for j in range(PIECES):
            cols = pl.ds(j * tile, tile)
            upstream = cin[m, :, cols].astype(F32)
            th = thb[m, :, cols]
            slope = 1.0 - th * th
            mix[m, pl.ds(0, rank), cols] = (upstream * slope).astype(BF16)
            total = jnp.sum(upstream * pre[m, :, cols].astype(F32), axis=0, keepdims=True)
            primal = cpin[m, :, cols] * slope - 2.0 * total * th * slope
            mixp[m, :, cols] = primal
            mix[m, pl.ds(rank, rows - rank), cols] = first_row(primal, rows - rank).astype(BF16)

    def backward(slots, together):
        for j in range(PIECES):
            cols = pl.ds(j * tile, tile)
            both = jnp.dot(blocks(mix, slots), wt[:, cols], preferred_element_type=F32)
            for i, slot in enumerate(slots):
                back = both[i * rows : (i + 1) * rows]
                cout[slot, :, cols] = (cin[slot, :, cols].astype(F32) + back[:rank]).astype(BF16)
                cpout[slot, :, cols] = (
                    (cpin[slot, :, cols] + back[rank : rank + 1]).astype(BF16).astype(F32)
                )
                if together or i == 0:
                    relayed_copy(slot, j, False).start()
        if together:
            for slot in slots:
                relayed_copy(slot, PIECES, False).start()
        else:
            relayed_copy(slots[0], PIECES, False).start()
            for slot in slots[1:]:
                for j in range(PIECES + 1):
                    relayed_copy(slot, j, False).start()

    heads = Scatter(place, head_refs, head_sems)
    sums = Scatter(place, layer_refs, layer_sems)

    def compact(tangent, primal):
        def take(cols):
            block = tangent[pl.ds(0, n_mb), pl.ds(0, rank), cols]
            rest = stacked_rows(lambda m: primal[m, :, cols], n_mb, 16, block.shape[2])
            return jnp.concatenate(
                [block.reshape(n_mb * rank, block.shape[2]), rest.astype(BF16)], axis=0
            )

        return take

    def each(count, body):
        lax.fori_loop(0, count, lambda n, _: (body(n), 0)[1], 0)

    @pl.when(last)
    def _():
        def group(g):
            slots = (2 * g, 2 * g + 1)
            forward(slots, True, False)
            objective(2 * g, 2)
            for slot in slots:
                mixed(slot)
            backward(slots, False)

        each(n_mb // 2, group)
        loss_in[core * chips + place.mp] = loss_out[...]
        lax.fori_loop(1, 2 * chips, lambda i, _: (loss_copy(i).start(), 0)[1], 0)
        sums.turn(compact(xin, pin))

    @pl.when(first)
    def _():
        each(n_mb, lambda m: forward((m,), False, True))
        sums.turn(compact(xin, pin))

        def back(m):
            await_relayed(m, False)
            mixed(m)

        each(n_mb, back)
        relays_left(True)

    @pl.when(place.carrier)
    def _():
        def slot_of(unit):
            return unit // 2 + lax.rem(unit, 2) * n_mb

        def forth(unit):
            forward((slot_of(unit),), True, True)

            @pl.when(lax.rem(unit, 2) == 1)
            def _():
                hand_over(0, slot_of(unit))

        each(2 * n_mb, forth)

        @pl.when(jnp.logical_not(late))
        def _():
            turned_into(wt, w)

        @pl.when(jnp.logical_not(late))
        def _():
            sums.turn(compact(xin, pin))

        relays_left(True)

        def back(unit):
            slot = slot_of(unit)
            await_relayed(slot, False)
            mixed(slot)
            backward((slot,), True)

            @pl.when(lax.rem(unit, 2) == 1)
            def _():
                hand_over(1, slot)

        each(2 * n_mb, back)

        @pl.when(late)
        def _():
            sums.turn(compact(xin, pin))

    @pl.when(jnp.logical_and(place.middle, core == 0))
    def _():
        for copy in handed(0):
            copy.wait_recv()
        sums.turn(compact(xin, pin))
        for copy in handed(1):
            copy.wait_recv()

    def section_copy(step, what):
        other = lax.rem(place.s + step, sections)
        if what == 0:
            return remote(head_out.at[other], head_land, zsend.at[0], zrecv.at[0], {"section": other})
        return remote(loss_sum, loss_land, zsend.at[1], zrecv.at[1], {"section": other})

    @pl.when(last)
    def _():
        heads.turn(compact(xout, pout))
        heads.right[...] = compact(cot, cotp)(slice(None))
        heads.products()

        def finish(q, value):
            per = out_width // sections
            for k in range(heads.half // per):
                head_out[q * (heads.half // per) + k] = value[:, k * per : (k + 1) * per]

        heads.run(finish)
        all_losses().wait_recv()
        loss_sum[...] = jnp.sum(loss_in[...], axis=0) * loss_scale

        def spread(i, _):
            section_copy(i, 0).start()
            section_copy(i, 1).start()
            return 0

        lax.fori_loop(1, sections, spread, 0)
        heads.drain()
        o_head[...] = head_out[sections - 1].astype(BF16)
        o_loss[...] = loss_sum[0:1, 0:1]

    sums.right[...] = compact(mix, mixp)(slice(None))
    sums.products()

    def layer_out(q):
        cols = pl.ds(q * sums.half, sums.half)
        return pltpu.make_async_copy(o_layer_buf.at[:, cols], o_layer.at[:, cols], stored.at[q])

    def finish_layer(q, value):
        o_layer_buf[:, pl.ds(q * sums.half, sums.half)] = value.astype(BF16)
        layer_out(q).start()

    sums.run(finish_layer)

    @pl.when(jnp.logical_not(last))
    def _():
        section_copy(1, 0).wait_recv()
        section_copy(1, 1).wait_recv()
        o_head[...] = head_land[...].astype(BF16)
        o_loss[...] = loss_land[0:1, 0:1]

    @pl.when(jnp.logical_not(first))
    def _():
        relays_left(False)

    @pl.when(place.carrier)
    def _():
        for kind in (0, 1):
            for copy in handed(kind):
                copy.wait_send()

    gather.drain()
    sums.drain()
    layer_out(0).wait()
    layer_out(1).wait()

    @pl.when(last)
    def _():
        all_counts().wait_send()
        all_losses().wait_send()
        for ref, n in ((head_out, 0), (loss_in, 1)):
            ref = ref.at[pl.ds(0, sections - 1)]
            remote(ref, ref, zsend.at[n], zrecv.at[n], {"section": place.nxt}).wait_send()


def scatter_scratch(rows, cols, depth, shared):
    half = cols // 2
    dma = pltpu.SemaphoreType.DMA
    part = (SIDE, SIDE, rows, cols)
    local = [] if shared else [pltpu.VMEM(part, BF16)]
    return [
        *local,
        pltpu.VMEM(part, BF16),
        *local,
        pltpu.VMEM((2, 2, 2, rows, half), BF16),
        pltpu.VMEM((2, 2, SIDE, rows, half), BF16),
        pltpu.VMEM((2, 2, rows // 2, half), BF16),
        pltpu.VMEM((2, 2, rows, half), BF16),
        pltpu.VMEM((2, SIDE, SIDE, rows, depth), BF16),
        pltpu.VMEM((depth, cols), BF16),
        dma((5,)), dma((2, SIDE)), dma((2, 2, 2)), dma((2, 2, SIDE)), dma((2, 2, 2)),
    ]


def local(
    inputs, tangents, targets, target_jac, rank_mask, batch_order, encoder, layers, head_weight
):
    n_mb, rank, _ = tangents.shape
    width = layers.shape[2]
    out_width = head_weight.shape[1]
    sections = lax.axis_size("section")
    chips = SIDE * SIDE
    own = width // (2 * chips)
    per = out_width // sections
    dma = pltpu.SemaphoreType.DMA
    vmem = pl.BlockSpec(memory_space=pltpu.VMEM)
    hbm = pl.BlockSpec(memory_space=pl.ANY)
    like = lambda a: pltpu.VMEM(a.shape, a.dtype)
    row = pltpu.VMEM((n_mb, 1, width), F32)
    rows = pltpu.VMEM((2 * n_mb, 1, width), F32)
    block = pltpu.VMEM((n_mb, ROWS, width), BF16)
    blocks = pltpu.VMEM((2 * n_mb, ROWS, width), BF16)
    send = pltpu.VMEM((2 * n_mb, rank, width), BF16)
    grad_layer, grad_head, loss = pl.pallas_call(
        functools.partial(step_kernel, sections, 1.0 / (lax.axis_size("dp") * n_mb * out_width)),
        out_shape=(
            jax.ShapeDtypeStruct((own, width), BF16),
            jax.ShapeDtypeStruct((own, per), BF16),
            jax.ShapeDtypeStruct((1, 1), F32),
        ),
        in_specs=[hbm] * 4 + [vmem] * 2 + [hbm] * 3,
        out_specs=(hbm, vmem, vmem),
        scratch_shapes=[
            like(inputs), like(tangents), like(targets), like(target_jac),
            like(layers[0]), like(head_weight),
            pltpu.VMEM((width, width), BF16),
            pltpu.VMEM((width, width), BF16),
            pltpu.VMEM((out_width, width), BF16),
            blocks, block, blocks,
            pltpu.VMEM((n_mb, ROWS, out_width), BF16),
            rows, row, send,
            rows, send, rows, send, rows, rows,
            pltpu.VMEM((n_mb, 1, out_width), F32),
            pltpu.VMEM((own, width), BF16),
            pltpu.VMEM((n_mb, ROWS, 1), F32),
            pltpu.VMEM((n_mb, 1, out_width), F32),
            pltpu.VMEM((8, 128), F32),
            pltpu.VMEM((chips, 8, 128), F32),
            pltpu.VMEM((8, 128), F32),
            pltpu.VMEM((2 * chips, 8, 128), F32),
            pltpu.VMEM((8, 128), F32),
            pltpu.VMEM((8, 128), F32),
            pltpu.VMEM((sections, own, per), F32),
            pltpu.VMEM((own, per), F32),
            dma((7,)), dma((2,)), dma((4,)), dma((2 * n_mb, 2)), dma((2 * n_mb, 2)),
            dma, dma((2, 4)), dma((2, SIDE, 4)), dma, dma,
            dma((1,)), dma((1,)), dma((1,)), dma((1,)), dma((2,)), dma((2,)), dma((4,)), dma((4,)),
            *scatter_scratch(own, width, n_mb * rank + 16, False),
            *scatter_scratch(own, out_width, n_mb * rank + 16, True),
        ],
        compiler_params=pltpu.CompilerParams(
            collective_id=0, has_side_effects=True, vmem_limit_bytes=67043328
        ),
        name="step",
    )(
        inputs, tangents, targets, target_jac, rank_mask, batch_order, encoder, layers[0],
        head_weight,
    )
    return grad_layer[None].astype(F32), grad_head.astype(F32), loss.reshape(())


def solution(mesh):
    in_specs = (
        P(("dp", "mp"), None),
        P(("dp", "mp"), None, None),
        P(("dp", "mp"), None),
        P(("dp", "mp"), None, None),
        P(("dp", "mp"), None),
        P(("dp", "mp"), None),
        P(),
        P("section", "mp", None),
        P(),
    )
    out_specs = (P("section", ("dp", "mp"), None), P(("dp", "mp"), "section"), P())
    return jax.shard_map(local, mesh=mesh, in_specs=in_specs, out_specs=out_specs, check_vma=False)
```

```python
import functools

import jax
import jax.numpy as jnp
from jax import lax
from jax.experimental import pallas as pl
from jax.experimental.pallas import tpu as pltpu
from jax.sharding import PartitionSpec as P

SIDE = 4
ROWS = 48
PIECES = 2
MESH = pl.DeviceIdType.MESH
BF16, F32 = jnp.bfloat16, jnp.float32


def first_row(row, height):
    rows = lax.broadcasted_iota(jnp.int32, (height, row.shape[1]), 0)
    return jnp.where(rows == 0, jnp.broadcast_to(row, (height, row.shape[1])), 0.0)


def stacked_rows(get_row, count, height, width):
    rows = lax.broadcasted_iota(jnp.int32, (height, width), 0)
    block = jnp.zeros((height, width), F32)
    for m in range(count):
        block = jnp.where(rows == m, jnp.broadcast_to(get_row(m), (height, width)), block)
    return block


class Place:
    def __init__(self, sections):
        self.sections = sections
        self.core = lax.axis_index("dp")
        self.s = lax.axis_index("section")
        self.mp = lax.axis_index("mp")
        self.y = self.mp // SIDE
        self.x = lax.rem(self.mp, SIDE)
        self.first = self.s == 0
        self.last = self.s == sections - 1
        self.middle = jnp.logical_not(jnp.logical_or(self.first, self.last))
        self.carrier = jnp.logical_and(self.middle, self.core == 1)
        self.nxt = lax.rem(self.s + 1, sections)
        self.prv = lax.rem(self.s + sections - 1, sections)

    def along(self, coordinate, steps):
        return lax.rem(coordinate + steps + SIDE, SIDE)

    def chip(self, axis, steps):
        if axis == 0:
            return self.y * SIDE + self.along(self.x, steps)
        return self.along(self.y, steps) * SIDE + self.x


def remote(src, dst, send, recv, device_id):
    return pltpu.make_async_remote_copy(
        src_ref=src, dst_ref=dst, send_sem=send, recv_sem=recv,
        device_id=device_id, device_id_type=MESH,
    )


def neighbours(place):
    for axis in (0, 1):
        for steps in (1, -1):
            yield {"mp": place.chip(axis, steps)}
    yield {"dp": 1 - place.core}
    for section in (place.nxt, place.prv):
        for core in (0, 1):
            yield {"dp": core, "section": section}


def knock(place):
    barrier = pltpu.get_barrier_semaphore()
    for device in neighbours(place):
        pl.semaphore_signal(barrier, inc=1, device_id=device, device_id_type=MESH)


def enter():
    pl.semaphore_wait(pltpu.get_barrier_semaphore(), 9)


class Gather:
    def __init__(self, place, shard, w, sems):
        self.p, self.shard, self.w = place, shard, w
        self.sent, self.recv1, self.recv2, self.dsent, self.dgot = sems
        self.depth = shard.shape[0]
        self.piece = self.depth // 4

    def rows(self, q, core, step1, step2, half):
        p = self.p
        dx, dy = (step1, step2) if q == 0 else (step2, step1)
        chip = p.along(p.y, dy) * SIDE + p.along(p.x, dx)
        start = chip * self.depth + core * (2 * self.piece) + q * self.piece
        length = self.piece
        if half is not None:
            length = self.piece // 2
            start = start + half * length
        return pl.ds(pl.multiple_of(start, length), length)

    def copy(self, q, phase, o, e):
        p = self.p
        axis = q if phase == 1 else 1 - q
        to = 1 if e in (0, 2) else -1
        back = {0: 0, 1: 0, 2: -1, 3: 1}[e]
        half = {0: None, 1: None, 2: 0, 3: 1}[e]
        step1, step2 = (back, 0) if phase == 1 else (o, back)
        dst = self.w.at[self.rows(q, p.core, step1, step2, half)]
        src = dst
        if step1 == 0 and step2 == 0:
            src = self.shard.at[pl.ds(pl.multiple_of(p.core * (2 * self.piece) + q * self.piece, self.piece), self.piece)]
        return remote(src, dst, self.sent, self.recv(phase, q, o, e), {"mp": p.chip(axis, to)})

    def recv(self, phase, q, o, e):
        return self.recv1.at[q, e] if phase == 1 else self.recv2.at[q, o % SIDE, e]

    def arrived(self, q, phase, o, e):
        p = self.p
        away = {0: -1, 1: 1, 2: -2, 3: 2}[e]
        half = {0: None, 1: None, 2: 0, 3: 1}[e]
        step1, step2 = (away, 0) if phase == 1 else (o, away)
        return self.p, q, step1, step2, half

    def wait(self, q, phase, o, e):
        p, q, step1, step2, half = self.arrived(q, phase, o, e)
        dst = self.w.at[self.rows(q, p.core, step1, step2, half)]
        remote(dst, dst, self.sent, self.recv(phase, q, o, e), {"mp": p.chip(0, 1)}).wait_recv()
        remote(dst, dst, self.dsent, self.dgot, {"dp": 1 - p.core}).start()

    def all_of(self, send, recv):
        ref = self.w.at[pl.ds(0, (SIDE * SIDE - 1) * 2 * self.piece)]
        return remote(ref, ref, send, recv, {"dp": 1 - self.p.core})

    def begin(self):
        for q in (0, 1):
            self.copy(q, 1, 0, 0).start()
            self.copy(q, 1, 0, 1).start()
        for q in (0, 1):
            self.copy(q, 2, 0, 0).start()
            self.copy(q, 2, 0, 1).start()
        p = self.p
        self.w[pl.ds(pl.multiple_of(p.mp * self.depth, self.depth), self.depth), :] = self.shard[...]

    def run(self):
        for q in (0, 1):
            self.wait(q, 1, 0, 0)
            self.copy(q, 1, 0, 2).start()
            self.wait(q, 1, 0, 1)
            self.copy(q, 1, 0, 3).start()
        for q in (0, 1):
            for o in (-1, 1):
                self.copy(q, 2, o, 0).start()
                self.copy(q, 2, o, 1).start()
        for q in (0, 1):
            self.wait(q, 2, 0, 0)
            self.copy(q, 2, 0, 2).start()
            self.wait(q, 2, 0, 1)
            self.copy(q, 2, 0, 3).start()
        for q in (0, 1):
            self.wait(q, 1, 0, 2)
            self.wait(q, 1, 0, 3)
            self.copy(q, 2, 2, 0).start()
            self.copy(q, 2, 2, 1).start()
        for o in (-1, 1, 2):
            for q in (0, 1):
                self.wait(q, 2, o, 0)
                self.copy(q, 2, o, 2).start()
                self.wait(q, 2, o, 1)
                self.copy(q, 2, o, 3).start()
        for o in (0, -1, 1, 2):
            for q in (0, 1):
                self.wait(q, 2, o, 2)
                self.wait(q, 2, o, 3)
        self.all_of(self.dsent, self.dgot).wait_recv()

    def drain(self):
        self.all_of(self.sent, self.dgot).wait_send()
        self.all_of(self.dsent, self.dgot).wait_send()


class Scatter:
    STEPS = (2, 1, -1, 0)

    def __init__(self, place, refs, sems):
        self.p = place
        self.gs, self.gd, self.g, self.l1, self.l2, self.l3, self.l4, self.turned, self.right = refs
        self.sent, self.drecv, self.recv, self.recv2, self.recv4 = sems
        self.half = self.g.shape[3] // 2

    def cols(self, q):
        return pl.ds(q * self.half, self.half)

    def order(self, q):
        p = self.p
        return [p.along(p.x if q == 0 else p.y, steps) for steps in self.STEPS]

    def block(self, q, first, second):
        return (first, second) if q == 0 else (second, first)

    def ring1(self, q, steps):
        p = self.p
        return p.along(p.y if q == 0 else p.x, steps)

    def group(self, q, k):
        at = self.ring1(q, self.STEPS[k])
        return (at, slice(None)) if q == 0 else (slice(None), at)

    def pair(self, q, first, low):
        if q == 0:
            return self.g.at[first, pl.ds(low, 2), :, self.cols(q)]
        return self.g.at[pl.ds(low, 2), first, :, self.cols(q)]

    def copy1(self, q, d):
        src = self.pair(q, self.ring1(q, 2), 2 * d)
        return remote(src, self.l1.at[q, d], self.sent.at[1], self.recv.at[0, q, d],
                      {"mp": self.p.chip(1 - q, 1 if d == 0 else -1)})

    def copy2(self, q, d, b):
        to = 1 if d == 0 else -1
        at = self.block(q, self.ring1(q, to), b)
        return remote(self.g.at[(*at, slice(None), self.cols(q))], self.l2.at[q, d, b],
                      self.sent.at[2], self.recv2.at[q, d, b], {"mp": self.p.chip(1 - q, to)})

    def copy3(self, q, d):
        a, b = self.block(q, self.ring1(q, 0), self.order(q)[0])
        n = self.g.shape[2] // 2
        return remote(self.g.at[a, b, pl.ds(d * n, n), self.cols(q)], self.l3.at[q, d],
                      self.sent.at[3], self.recv.at[1, q, d],
                      {"mp": self.p.chip(q, 1 if d == 0 else -1)})

    def copy4(self, q, d, h):
        a, b = self.block(q, self.ring1(q, 0), self.order(q)[1 + d])
        n = self.g.shape[2] // 2
        rows = pl.ds(h * n, n)
        return remote(self.g.at[a, b, rows, self.cols(q)], self.l4.at[q, d, rows],
                      self.sent.at[4], self.recv4.at[q, d, h],
                      {"mp": self.p.chip(q, 1 if d == 0 else -1)})

    def exchange(self, q, k):
        index = (*self.group(q, k), slice(None), self.cols(q))
        return remote(self.gs.at[index], self.gd.at[index], self.sent.at[0], self.drecv.at[q, k],
                      {"dp": 1 - self.p.core})

    def turn(self, left):
        per = self.g.shape[1] * self.g.shape[2]

        def one(n, _):
            block = left(pl.ds(pl.multiple_of(n * per, per), per)).T
            self.turned[n // SIDE, lax.rem(n, SIDE)] = block.reshape(SIDE, self.g.shape[2], block.shape[1])
            return 0

        lax.fori_loop(0, 2 * SIDE, one, 0)

    def product(self, core, q, k):
        rows = self.turned[(core, *self.group(q, k))]
        rows = rows.reshape(-1, rows.shape[2])
        value = jnp.dot(rows, self.right[:, self.cols(q)], preferred_element_type=F32)
        return value.reshape(SIDE, self.g.shape[2], self.half)

    def other(self, q, k):
        index = (*self.group(q, k), slice(None), self.cols(q))
        self.gs[index] = self.product(1 - self.p.core, q, k).astype(BF16)
        self.exchange(q, k).start()

    def own(self, q, k):
        index = (*self.group(q, k), slice(None), self.cols(q))
        value = self.product(self.p.core, q, k)
        self.exchange(q, k).wait_recv()
        self.g[index] = (value + self.gd[index].astype(F32)).astype(BF16)
        if k == 0:
            self.copy1(q, 0).start()
            self.copy1(q, 1).start()
        elif k < 3:
            d = k - 1
            self.copy2(q, d, 2 - 2 * d).start()
            self.copy2(q, d, 3 - 2 * d).start()

    def products(self):
        parts = [(q, k) for k in range(SIDE) for q in (0, 1)]
        ahead = 3
        for n in range(len(parts) + ahead):
            if n < len(parts):
                self.other(*parts[n])
            if n >= ahead:
                self.own(*parts[n - ahead])

    def add(self, index, value):
        self.g[index] = (self.g[index].astype(F32) + value.astype(F32)).astype(BF16)

    def arrived(self, q, k):
        b = self.order(q)[k]
        self.copy2(q, 0, b).wait_recv()
        self.copy2(q, 1, b).wait_recv()
        return self.l2[q, 0, b].astype(F32) + self.l2[q, 1, b].astype(F32)

    def run(self, finish):
        n = self.g.shape[2] // 2
        index = lambda q, k: (*self.block(q, self.ring1(q, 0), self.order(q)[k]), slice(None), self.cols(q))
        for d in (0, 1):
            for q in (0, 1):
                self.copy1(q, d).wait_recv()
                first = self.ring1(q, 1 if d == 0 else -1)
                for k in (0, 1):
                    a, b = self.block(q, first, 2 * d + k)
                    self.add((a, b, slice(None), self.cols(q)), self.l1[q, d, k])
                far = self.order(q)[0]
                low = jnp.where(far // 2 == d, far, 2 * d)
                self.copy2(q, d, low).start()
                self.copy2(q, d, 4 * d + 1 - low).start()
        for q in (0, 1):
            self.add(index(q, 0), self.arrived(q, 0))
            self.copy3(q, 0).start()
            self.copy3(q, 1).start()
        for d in (0, 1):
            for q in (0, 1):
                self.add(index(q, 1 + d), self.arrived(q, 1 + d))
                self.copy4(q, d, 1 - d).start()
        for d in (0, 1):
            for q in (0, 1):
                a, b, _, cols = index(q, 1 + d)
                self.copy3(q, d).wait_recv()
                self.add((a, b, pl.ds(d * n, n), cols), self.l3[q, d])
                self.copy4(q, d, d).start()
        for q in (0, 1):
            value = self.g[index(q, 3)].astype(F32) + self.arrived(q, 3)
            for d in (0, 1):
                self.copy4(q, d, 0).wait_recv()
                self.copy4(q, d, 1).wait_recv()
            finish(q, value + self.l4[q, 0].astype(F32) + self.l4[q, 1].astype(F32))

    def drain(self):
        for n, ref in enumerate((self.gd, self.l1, self.l2, self.l3, self.l4)):
            remote(ref, ref, self.sent.at[n], self.drecv.at[0, 0], {"dp": 1 - self.p.core}).wait_send()


def step_kernel(sections, loss_scale, *refs):
    (
        h_inputs, h_tangents, h_targets, h_target_jac, mask, batch_order, h_encoder, h_shard, h_head,
        o_layer, o_head, o_loss,
        inputs, tangents, targets, target_jac, shard, head,
        w, wt, head_t, xin, xout, mix, cot, pin, pout, pre, thb, cin, cpin, cout, cpout, mixp, cotp,
        o_layer_buf, head_buf, loss_buf, coef, wantp, count_out, count_in, loss_out, loss_in, loss_sum, loss_land, head_out, head_land,
        loads, stored, relayed, frecv, brecv,
        gsent, grecv1, grecv2, dsent, dgot,
        csend, crecv, lsend, lrecv, zsend, zrecv, hsend, hrecv,
        *scatter,
    ) = refs
    layer_refs, layer_sems = scatter[:9], scatter[9:14]
    n_mb, rows, width = xout.shape
    rank = cin.shape[1]
    out_width = head.shape[1]
    part = pl.ds(0, out_width)
    head_refs = (
        layer_refs[0].at[:, :, :, part], scatter[14], layer_refs[2].at[:, :, :, part], *scatter[15:21]
    )
    head_sems = scatter[21:26]
    tile = width // PIECES
    place = Place(sections)
    s, core, first, last = place.s, place.core, place.first, place.last
    chips = SIDE * SIDE

    encoder = head_t.at[pl.ds(0, h_encoder.shape[0])]

    def load(n):
        pairs = (
            (h_shard, shard), (h_inputs, inputs), (h_tangents, tangents), (h_encoder, encoder),
            (h_targets, targets), (h_target_jac, target_jac), (h_head, head),
        )
        return pltpu.make_async_copy(pairs[n][0], pairs[n][1], loads.at[n])

    for n in range(7):
        load(n).start()
    knock(place)

    load(0).wait()
    enter()
    gather = Gather(place, shard, w, (gsent, grecv1, grecv2, dsent, dgot))
    gather.begin()

    @pl.when(first)
    def _():
        for n in (1, 2, 3):
            load(n).wait()
        primal = inputs[...].astype(F32)
        for m in range(n_mb):
            lhs = jnp.concatenate(
                [tangents[m], first_row(primal[m : m + 1], rows - rank).astype(BF16)], axis=0
            )
            lifted = jnp.dot(lhs, encoder[...], preferred_element_type=F32).astype(BF16)
            xin[m] = lifted
            pin[m] = lifted[rank:].astype(F32)[0:1]

    gather.run()
    for n in (4, 5, 6):
        load(n).wait()

    @pl.when(jnp.logical_not(first))
    def _():
        for n in (1, 2, 3):
            load(n).wait()

    def count_copy(step):
        other = lax.rem(place.mp + step, chips)
        return remote(count_out, count_in.at[place.mp], csend.at[0], crecv.at[0], {"mp": other})

    def all_counts():
        ref = count_in.at[pl.ds(0, chips - 1)]
        return remote(ref, ref, csend.at[0], crecv.at[0], {"dp": 1 - core})

    def all_losses():
        ref = loss_in.at[pl.ds(0, 2 * chips - 1)]
        return remote(ref, ref, lsend.at[0], lrecv.at[0], {"dp": 1 - core})

    def turned_into(target, source):
        high, wide = source.shape
        step = 512 if high % 512 == 0 and wide % 512 == 0 else min(high, wide)
        count = wide // step

        def turn(n, _):
            a = pl.ds(pl.multiple_of((n // count) * step, step), step)
            b = pl.ds(pl.multiple_of(lax.rem(n, count) * step, step), step)
            target[b, a] = source[a, b].T
            return 0

        lax.fori_loop(0, (high // step) * count, turn, 0)

    @pl.when(last)
    def _():
        totals = 1.0 + jnp.sum(mask[...].astype(F32), axis=1, keepdims=True)
        where = lax.broadcasted_iota(jnp.int32, (n_mb, n_mb), 0) == jnp.broadcast_to(
            batch_order[...], (n_mb, n_mb)
        )
        where = where.astype(F32)
        count_out[...] = jnp.zeros_like(count_out)
        count_out[0:1, 0:n_mb] = jnp.sum(where * totals, axis=0, keepdims=True)
        count_in[place.mp] = count_out[...]
        lax.fori_loop(1, chips, lambda i, _: (count_copy(i).start(), 0)[1], 0)
        turned_into(head_t, head)
        all_counts().wait_recv()
        counts = jnp.sum(count_in[...], axis=0)[0:1, 0:n_mb]
        inverse = 1.0 / jnp.sum(where * counts, axis=1, keepdims=True)
        row = lax.broadcasted_iota(jnp.int32, (rows, 1), 0)
        ranks = totals.astype(jnp.int32) - 1
        primal_wanted = targets[...].astype(F32)
        for m in range(n_mb):
            present = jnp.logical_or(row < ranks[m : m + 1], row == rank)
            coef[m] = jnp.where(present, inverse[m : m + 1], 0.0)
            wantp[m] = primal_wanted[m : m + 1]
        loss_out[...] = jnp.zeros_like(loss_out)

    late = s >= sections // 2

    @pl.when(jnp.logical_and(late, jnp.logical_or(last, place.carrier)))
    def _():
        turned_into(wt, w)

    def onward(slot, end):
        m = lax.rem(slot, n_mb)
        away = jnp.logical_or(slot >= n_mb, jnp.logical_and(jnp.logical_not(place.middle), core == 0))
        to_own = jnp.logical_and(away, end)
        taker = jnp.where(to_own, 0, 1)
        return taker, m + jnp.where(jnp.logical_and(away, jnp.logical_not(end)), n_mb, 0)

    def relayed_copy(slot, j, forth):
        to = place.nxt if forth else place.prv
        taker, there = onward(slot, to == (sections - 1 if forth else 0))
        device = {"dp": taker, "section": to}
        recv = frecv if forth else brecv
        kind = 0 if forth else 2
        if j == PIECES:
            landing = pin if forth else cpin
            return remote(cpout.at[slot], landing.at[there], relayed.at[kind + 1], recv.at[there, 1], device)
        cols = pl.ds(j * tile, tile)
        landing = xin.at[there, pl.ds(0, rank), cols] if forth else cin.at[there, :, cols]
        return remote(cout.at[slot, :, cols], landing, relayed.at[kind], recv.at[there, 0], device)

    def await_relayed(slot, forth):
        recv = frecv if forth else brecv
        ref = xin.at[slot, pl.ds(0, rank)] if forth else cin.at[slot]
        remote(ref, ref, relayed.at[0], recv.at[slot, 0], {"section": place.nxt}).wait_recv()
        ref = pin.at[slot] if forth else cpin.at[slot]
        remote(ref, ref, relayed.at[1], recv.at[slot, 1], {"section": place.nxt}).wait_recv()

    def relays_left(forth):
        kind = 0 if forth else 2
        for count, when in ((n_mb, jnp.logical_not(place.middle)), (2 * n_mb, place.carrier)):

            @pl.when(when)
            def _(count=count):
                for n, ref in ((kind, cin), (kind + 1, cpin)):
                    ref = ref.at[pl.ds(0, count)]
                    remote(ref, ref, relayed.at[n], frecv.at[0, 0], {"section": place.nxt}).wait_send()

    def hand_over(kind, slot):
        to = slot - n_mb
        pairs = ((xin, pin), (mix, mixp))[kind]
        for n, ref in enumerate(pairs):
            sem = 2 * kind + n
            remote(ref.at[slot], ref.at[to], hsend.at[sem], hrecv.at[sem], {"dp": 1 - core}).start()

    def handed(kind):
        pairs = ((xin, pin), (mix, mixp))[kind]
        for n, ref in enumerate(pairs):
            ref = ref.at[pl.ds(0, n_mb)]
            sem = 2 * kind + n
            yield remote(ref, ref, hsend.at[sem], hrecv.at[sem], {"dp": 1 - core})

    def blocks(ref, slots):
        return jnp.concatenate([ref[slot] for slot in slots], axis=0)

    def forward(slots, arriving, sending):
        if arriving:
            for slot in slots:
                await_relayed(slot, True)
                xin[slot, pl.ds(rank, rows - rank), :] = first_row(pin[slot], rows - rank).astype(BF16)
        for j in range(PIECES):
            cols = pl.ds(j * tile, tile)
            both = jnp.dot(blocks(xin, slots), w[:, cols], preferred_element_type=F32)
            for i, slot in enumerate(slots):
                acc = both[i * rows : i * rows + rows]
                th = jnp.tanh(acc[rank : rank + 1, :])
                slope = 1.0 - th * th
                tangent = acc[:rank, :]
                pre[slot, :, cols] = tangent.astype(BF16)
                thb[slot, :, cols] = th
                moved = xin[slot, pl.ds(0, rank), cols].astype(F32) + slope * tangent
                primal = (pin[slot, :, cols] + th).astype(BF16).astype(F32)
                if sending:
                    cout[slot, :, cols] = moved.astype(BF16)
                    cpout[slot, :, cols] = primal
                    relayed_copy(slot, j, True).start()
                else:
                    pout[slot, :, cols] = primal
                    xout[slot, pl.ds(0, rank), cols] = moved.astype(BF16)
                    xout[slot, pl.ds(rank, rows - rank), cols] = first_row(primal, rows - rank).astype(BF16)
        if sending:
            for slot in slots:
                relayed_copy(slot, PIECES, True).start()

    def loss_copy(step):
        plane = 2 * chips
        me = core * chips + place.mp
        other = lax.rem(me + step, plane)
        return remote(
            loss_out, loss_in.at[me], lsend.at[0], lrecv.at[0],
            {"dp": other // chips, "mp": lax.rem(other, chips)},
        )

    def objective(m, span):
        step = min(256, out_width)
        total = jnp.zeros((1, 1), F32)
        for n in range(out_width // step):
            cols = pl.ds(n * step, step)
            outputs = jnp.dot(
                xout[pl.ds(m, span)].reshape(span * rows, width), head[:, cols],
                preferred_element_type=F32,
            )
            for i in range(span):
                wanted = jnp.concatenate(
                    [
                        target_jac[m + i, :, cols].astype(F32),
                        first_row(wantp[m + i, :, cols], rows - rank),
                    ],
                    axis=0,
                )
                mismatch = outputs[i * rows : (i + 1) * rows] - wanted
                weighted = coef[m + i] * mismatch
                total = total + jnp.sum(
                    jnp.sum(weighted * mismatch, axis=0, keepdims=True), axis=1, keepdims=True
                )
                rounded = (2.0 * weighted).astype(BF16)
                cot[m + i, :, cols] = rounded
                cotp[m + i, :, cols] = rounded[rank:].astype(F32)[0:1]
        loss_out[...] = loss_out[...] + jnp.broadcast_to(total, loss_out.shape)
        for j in range(PIECES):
            cols = pl.ds(j * tile, tile)
            grads = jnp.dot(
                cot[pl.ds(m, span)].reshape(span * rows, out_width), head_t[:, cols],
                preferred_element_type=F32,
            ).astype(BF16)
            for i in range(span):
                cin[m + i, :, cols] = grads[i * rows : i * rows + rank, :]
                cpin[m + i, :, cols] = grads[i * rows + rank : (i + 1) * rows, :].astype(F32)[0:1]

    def mixed(m):
        for j in range(PIECES):
            cols = pl.ds(j * tile, tile)
            upstream = cin[m, :, cols].astype(F32)
            th = thb[m, :, cols]
            slope = 1.0 - th * th
            mix[m, pl.ds(0, rank), cols] = (upstream * slope).astype(BF16)
            total = jnp.sum(upstream * pre[m, :, cols].astype(F32), axis=0, keepdims=True)
            primal = cpin[m, :, cols] * slope - 2.0 * total * th * slope
            mixp[m, :, cols] = primal
            mix[m, pl.ds(rank, rows - rank), cols] = first_row(primal, rows - rank).astype(BF16)

    def backward(slots, together):
        for j in range(PIECES):
            cols = pl.ds(j * tile, tile)
            both = jnp.dot(blocks(mix, slots), wt[:, cols], preferred_element_type=F32)
            for i, slot in enumerate(slots):
                back = both[i * rows : (i + 1) * rows]
                cout[slot, :, cols] = (cin[slot, :, cols].astype(F32) + back[:rank]).astype(BF16)
                cpout[slot, :, cols] = (
                    (cpin[slot, :, cols] + back[rank : rank + 1]).astype(BF16).astype(F32)
                )
                if together or i == 0:
                    relayed_copy(slot, j, False).start()
        if together:
            for slot in slots:
                relayed_copy(slot, PIECES, False).start()
        else:
            relayed_copy(slots[0], PIECES, False).start()
            for slot in slots[1:]:
                for j in range(PIECES + 1):
                    relayed_copy(slot, j, False).start()

    heads = Scatter(place, head_refs, head_sems)
    sums = Scatter(place, layer_refs, layer_sems)

    def compact(tangent, primal):
        def take(cols):
            block = tangent[pl.ds(0, n_mb), pl.ds(0, rank), cols]
            rest = stacked_rows(lambda m: primal[m, :, cols], n_mb, 16, block.shape[2])
            return jnp.concatenate(
                [block.reshape(n_mb * rank, block.shape[2]), rest.astype(BF16)], axis=0
            )

        return take

    def each(count, body):
        lax.fori_loop(0, count, lambda n, _: (body(n), 0)[1], 0)

    @pl.when(last)
    def _():
        def group(g):
            slots = (2 * g, 2 * g + 1)
            forward(slots, True, False)
            objective(2 * g, 2)
            for slot in slots:
                mixed(slot)
            backward(slots, False)

        each(n_mb // 2, group)
        loss_in[core * chips + place.mp] = loss_out[...]
        lax.fori_loop(1, 2 * chips, lambda i, _: (loss_copy(i).start(), 0)[1], 0)
        sums.turn(compact(xin, pin))

    @pl.when(first)
    def _():
        each(n_mb, lambda m: forward((m,), False, True))
        sums.turn(compact(xin, pin))

        def back(m):
            await_relayed(m, False)
            mixed(m)

        each(n_mb, back)
        relays_left(True)

    @pl.when(place.carrier)
    def _():
        def slot_of(unit):
            return unit // 2 + lax.rem(unit, 2) * n_mb

        def forth(unit):
            forward((slot_of(unit),), True, True)

            @pl.when(lax.rem(unit, 2) == 1)
            def _():
                hand_over(0, slot_of(unit))

        each(2 * n_mb, forth)

        @pl.when(jnp.logical_not(late))
        def _():
            turned_into(wt, w)

        @pl.when(jnp.logical_not(late))
        def _():
            sums.turn(compact(xin, pin))

        relays_left(True)

        def back(unit):
            slot = slot_of(unit)
            await_relayed(slot, False)
            mixed(slot)
            backward((slot,), True)

            @pl.when(lax.rem(unit, 2) == 1)
            def _():
                hand_over(1, slot)

        each(2 * n_mb, back)

        @pl.when(late)
        def _():
            sums.turn(compact(xin, pin))

    @pl.when(jnp.logical_and(place.middle, core == 0))
    def _():
        for copy in handed(0):
            copy.wait_recv()
        sums.turn(compact(xin, pin))
        for copy in handed(1):
            copy.wait_recv()

    def section_copy(step, what):
        other = lax.rem(place.s + step, sections)
        if what == 0:
            return remote(head_out.at[other], head_land, zsend.at[0], zrecv.at[0], {"section": other})
        return remote(loss_sum, loss_land, zsend.at[1], zrecv.at[1], {"section": other})

    @pl.when(last)
    def _():
        heads.turn(compact(xout, pout))
        heads.right[...] = compact(cot, cotp)(slice(None))
        heads.products()

        def finish(q, value):
            per = out_width // sections
            for k in range(heads.half // per):
                head_out[q * (heads.half // per) + k] = value[:, k * per : (k + 1) * per]

        heads.run(finish)
        all_losses().wait_recv()
        loss_sum[...] = jnp.sum(loss_in[...], axis=0) * loss_scale

        def spread(i, _):
            section_copy(i, 0).start()
            section_copy(i, 1).start()
            return 0

        lax.fori_loop(1, sections, spread, 0)
        heads.drain()
        head_buf[...] = head_out[sections - 1].astype(BF16)
        loss_buf[...] = loss_sum[0:1, 0:1]

    def head_store():
        return pltpu.make_async_copy(head_buf, o_head, stored.at[2])

    def loss_store():
        return pltpu.make_async_copy(loss_buf, o_loss, stored.at[3])

    sums.right[...] = compact(mix, mixp)(slice(None))
    sums.products()

    @pl.when(jnp.logical_not(last))
    def _():
        section_copy(1, 0).wait_recv()
        section_copy(1, 1).wait_recv()
        head_buf[...] = head_land[...].astype(BF16)
        loss_buf[...] = loss_land[0:1, 0:1]

    head_store().start()
    loss_store().start()

    def layer_out(q):
        cols = pl.ds(q * sums.half, sums.half)
        return pltpu.make_async_copy(o_layer_buf.at[:, cols], o_layer.at[:, cols], stored.at[q])

    def finish_layer(q, value):
        o_layer_buf[:, pl.ds(q * sums.half, sums.half)] = value.astype(BF16)
        layer_out(q).start()

    sums.run(finish_layer)

    @pl.when(jnp.logical_not(first))
    def _():
        relays_left(False)

    @pl.when(place.carrier)
    def _():
        for kind in (0, 1):
            for copy in handed(kind):
                copy.wait_send()

    gather.drain()
    sums.drain()
    layer_out(0).wait()
    layer_out(1).wait()
    head_store().wait()
    loss_store().wait()

    @pl.when(last)
    def _():
        all_counts().wait_send()
        all_losses().wait_send()
        for ref, n in ((head_out, 0), (loss_in, 1)):
            ref = ref.at[pl.ds(0, sections - 1)]
            remote(ref, ref, zsend.at[n], zrecv.at[n], {"section": place.nxt}).wait_send()


def scatter_scratch(rows, cols, depth, shared):
    half = cols // 2
    dma = pltpu.SemaphoreType.DMA
    part = (SIDE, SIDE, rows, cols)
    local = [] if shared else [pltpu.VMEM(part, BF16)]
    return [
        *local,
        pltpu.VMEM(part, BF16),
        *local,
        pltpu.VMEM((2, 2, 2, rows, half), BF16),
        pltpu.VMEM((2, 2, SIDE, rows, half), BF16),
        pltpu.VMEM((2, 2, rows // 2, half), BF16),
        pltpu.VMEM((2, 2, rows, half), BF16),
        pltpu.VMEM((2, SIDE, SIDE, rows, depth), BF16),
        pltpu.VMEM((depth, cols), BF16),
        dma((5,)), dma((2, SIDE)), dma((2, 2, 2)), dma((2, 2, SIDE)), dma((2, 2, 2)),
    ]


def local(
    inputs, tangents, targets, target_jac, rank_mask, batch_order, encoder, layers, head_weight
):
    n_mb, rank, _ = tangents.shape
    width = layers.shape[2]
    out_width = head_weight.shape[1]
    sections = lax.axis_size("section")
    chips = SIDE * SIDE
    own = width // (2 * chips)
    per = out_width // sections
    dma = pltpu.SemaphoreType.DMA
    vmem = pl.BlockSpec(memory_space=pltpu.VMEM)
    hbm = pl.BlockSpec(memory_space=pl.ANY)
    like = lambda a: pltpu.VMEM(a.shape, a.dtype)
    row = pltpu.VMEM((n_mb, 1, width), F32)
    rows = pltpu.VMEM((2 * n_mb, 1, width), F32)
    block = pltpu.VMEM((n_mb, ROWS, width), BF16)
    blocks = pltpu.VMEM((2 * n_mb, ROWS, width), BF16)
    send = pltpu.VMEM((2 * n_mb, rank, width), BF16)
    grad_layer, grad_head, loss = pl.pallas_call(
        functools.partial(step_kernel, sections, 1.0 / (lax.axis_size("dp") * n_mb * out_width)),
        out_shape=(
            jax.ShapeDtypeStruct((own, width), BF16),
            jax.ShapeDtypeStruct((own, per), BF16),
            jax.ShapeDtypeStruct((1, 1), F32),
        ),
        in_specs=[hbm] * 4 + [vmem] * 2 + [hbm] * 3,
        out_specs=(hbm, hbm, hbm),
        scratch_shapes=[
            like(inputs), like(tangents), like(targets), like(target_jac),
            like(layers[0]), like(head_weight),
            pltpu.VMEM((width, width), BF16),
            pltpu.VMEM((width, width), BF16),
            pltpu.VMEM((out_width, width), BF16),
            blocks, block, blocks,
            pltpu.VMEM((n_mb, ROWS, out_width), BF16),
            rows, row, send,
            rows, send, rows, send, rows, rows,
            pltpu.VMEM((n_mb, 1, out_width), F32),
            pltpu.VMEM((own, width), BF16),
            pltpu.VMEM((own, per), BF16),
            pltpu.VMEM((1, 1), F32),
            pltpu.VMEM((n_mb, ROWS, 1), F32),
            pltpu.VMEM((n_mb, 1, out_width), F32),
            pltpu.VMEM((8, 128), F32),
            pltpu.VMEM((chips, 8, 128), F32),
            pltpu.VMEM((8, 128), F32),
            pltpu.VMEM((2 * chips, 8, 128), F32),
            pltpu.VMEM((8, 128), F32),
            pltpu.VMEM((8, 128), F32),
            pltpu.VMEM((sections, own, per), F32),
            pltpu.VMEM((own, per), F32),
            dma((7,)), dma((4,)), dma((4,)), dma((2 * n_mb, 2)), dma((2 * n_mb, 2)),
            dma, dma((2, 4)), dma((2, SIDE, 4)), dma, dma,
            dma((1,)), dma((1,)), dma((1,)), dma((1,)), dma((2,)), dma((2,)), dma((4,)), dma((4,)),
            *scatter_scratch(own, width, n_mb * rank + 16, False),
            *scatter_scratch(own, out_width, n_mb * rank + 16, True),
        ],
        compiler_params=pltpu.CompilerParams(
            collective_id=0, has_side_effects=True, vmem_limit_bytes=67043328,
        ),
        name="step",
    )(
        inputs, tangents, targets, target_jac, rank_mask, batch_order, encoder, layers[0],
        head_weight,
    )
    return grad_layer[None].astype(F32), grad_head.astype(F32), loss.reshape(())


def solution(mesh):
    in_specs = (
        P(("dp", "mp"), None),
        P(("dp", "mp"), None, None),
        P(("dp", "mp"), None),
        P(("dp", "mp"), None, None),
        P(("dp", "mp"), None),
        P(("dp", "mp"), None),
        P(),
        P("section", "mp", None),
        P(),
    )
    out_specs = (P("section", ("dp", "mp"), None), P(("dp", "mp"), "section"), P())
    return jax.shard_map(local, mesh=mesh, in_specs=in_specs, out_specs=out_specs, check_vma=False)
```
